32 devices in a mesh: wide: 16 (over z, y, x), narrow: 2 (over core).
Axes of the slice: x: 2, y: 2, z: 4, core: 2. Of those that a mesh axis runs over, the one named last changes fastest.
Arguments:
- inputs: float32 [16, 64, 16, 128], P(None, 'wide', 'narrow'), may hold values from -100 to 100
- old_basis: float32 [256, 64, 16, 128], P(None, 'wide', 'narrow'), may hold values from -12 to 12
- conductance: float32 [64, 16, 128], P('wide', 'narrow'), may hold values from 0.5 to 2
- shifts: float32 [3], replicated, may hold values from 0.2 to 4
Outputs:
- new_columns: float32 [48, 64, 16, 128], P(None, 'wide', 'narrow')
- coefficients: float32 [256, 48], replicated
- col_scale: float32 [48], replicated
The draws below stay inside these ranges and needn't reach their ends.
All inputs are finite; a program needn't handle non-finite values.
Results may differ from the reference program's by a relative error of at most 0.00011.
Values sent between devices are 32-bit elements; how exact they have to be, the bound alone decides.
No kernel may reach another device: no remote copies, remote signals or barrier semaphores. Data moves between devices by JAX's collectives and lax.ppermute only.
A program may use at most 64 MiB of HBM per device.

```python
import math
import jax
import jax.numpy as jnp
from jax import lax

CZ = 128
INPUTS = 16
SHIFTS = 3
BASIS = 256
ITERS = 4
NX = 64
NY = 16


def shared_inputs(key):
    base = jax.random.normal(jax.random.fold_in(key, 11), (INPUTS, NX, NY, CZ), jnp.float32)
    base = jnp.clip(base, -6.0, 6.0)
    position = jnp.arange(NX, dtype=jnp.float32) / max(NX - 1, 1)
    ramp = jnp.exp(1.386 * position)[None, :, None, None]
    base = base * ramp
    return base


def draw_inputs(key, part):
    return shared_inputs(key)


def draw_old_basis(key, part):
    base = shared_inputs(key)
    mixing = 0.25 * jax.random.normal(jax.random.fold_in(key, 12), (BASIS, INPUTS), jnp.float32)
    noise = jnp.clip(jax.random.normal(jax.random.fold_in(key, 13), (BASIS, NX, NY, CZ), jnp.float32), -6.0, 6.0)
    shared = jnp.einsum('bm,mxyz->bxyz', mixing, base)
    return jnp.clip(0.25 * shared + 0.9 * noise, -12.0, 12.0)


def level_of(own_key, dims, shards, low, top_value):
    factor_of, own = 1.0, jax.random.fold_in(own_key, 6)
    for axis_at, blocks in shards:
        heights = jnp.exp(jax.random.uniform(jax.random.fold_in(own, axis_at), (blocks,), jnp.float32, low / len(shards), top_value / len(shards)))
        factor_of = factor_of * jnp.repeat(heights, dims[axis_at] // blocks).reshape([-1 if axis == axis_at else 1 for axis in range(len(dims))])
    return factor_of


def setup_inputs(seed: int = 0) -> dict:
    key_of = jax.random.split(jax.random.key(seed), 5)
    inputs = draw_inputs(jax.random.fold_in(key_of[4], 71), 0)
    old_basis = draw_old_basis(jax.random.fold_in(key_of[4], 71), 0)
    conductance = jnp.clip(jnp.exp(math.log(2.0) - 1.3862944 * jax.random.uniform(key_of[2], (NX, NY, CZ), jnp.float32) ** level_of(key_of[2], (NX, NY, CZ), ((0, 16), (1, 2)), -0.2, 0.2)), 0.5, 2.0)
    shifts = jnp.clip(jnp.exp(jax.random.uniform(key_of[3], (SHIFTS,), jnp.float32, math.log(0.2), math.log(4.0))), 0.2, 4.0)
    return dict(inputs=inputs, old_basis=old_basis, conductance=conductance, shifts=shifts)


def operate(values, conductance, shift_col):
    padded = jnp.pad(values, ((0, 0), (1, 1), (1, 1), (1, 1)))
    beside_all = padded[:, 2:, 1:-1, 1:-1] + padded[:, :-2, 1:-1, 1:-1]
    beside_all = beside_all + padded[:, 1:-1, 2:, 1:-1] + padded[:, 1:-1, :-2, 1:-1]
    beside_all = beside_all + padded[:, 1:-1, 1:-1, 2:] + padded[:, 1:-1, 1:-1, :-2]
    return conductance[None] * (6.0 * values - beside_all) + shift_col[:, None, None, None] * values

def spread(coef):
    return coef[:, None, None, None]

def reference(inputs, old_basis, conductance, shifts):
    total_cells = NX * NY * CZ

    def inner_mean(left, right):
        return lax.optimization_barrier(jnp.sum(left * right, axis=(1, 2, 3))) / total_cells
    shift_col = jnp.repeat(shifts, INPUTS)
    shadow = jnp.tile(inputs, (SHIFTS, 1, 1, 1))
    solution = jnp.zeros_like(shadow)
    residual = shadow
    search = shadow
    rho_now = inner_mean(shadow, shadow)
    for iteration in range(ITERS):
        search_image = operate(search, conductance, shift_col)
        step_alpha = rho_now / inner_mean(shadow, search_image)
        halfway = residual - spread(step_alpha) * search_image
        halfway_image = operate(halfway, conductance, shift_col)
        step_omega = inner_mean(halfway_image, halfway) / (inner_mean(halfway_image, halfway_image) + 1e-06)
        solution = solution + spread(step_alpha) * search + spread(step_omega) * halfway
        residual = halfway - spread(step_omega) * halfway_image
        rho_next = inner_mean(shadow, residual)
        step_beta = rho_next / rho_now * (step_alpha / step_omega)
        search = residual + spread(step_beta) * (search - spread(step_omega) * search_image)
        rho_now = rho_next
    columns = shadow.shape[0]
    vflat = old_basis.reshape(BASIS, -1)
    wflat = solution.reshape(columns, -1)
    high = lax.Precision.HIGHEST
    first_coef = jnp.einsum('bc,kc->bk', vflat, wflat, precision=high) / total_cells
    once = wflat - jnp.einsum('bk,bc->kc', first_coef, vflat, precision=high)
    second_coef = jnp.einsum('bc,kc->bk', vflat, once, precision=high) / total_cells
    twice = once - jnp.einsum('bk,bc->kc', second_coef, vflat, precision=high)
    col_scale = jnp.sqrt(lax.optimization_barrier(jnp.sum(twice * twice, axis=1)) / total_cells + 1e-06)
    new_columns = (twice / col_scale[:, None]).reshape(solution.shape)
    return (new_columns, first_coef + second_coef, col_scale)
```

```python
import functools
import math

import jax
import jax.numpy as jnp
from jax import lax
from jax.experimental import pallas as pl
from jax.experimental.pallas import tpu as pltpu
from jax.sharding import PartitionSpec as P

ITERS = 4
AXES = ("wide", "narrow")
SUB, LANE = 8, 128


def spread(coef):
    return coef[:, None, None, None]


def reduced(partial):
    count = lax.axis_size(AXES)
    copies = jnp.broadcast_to(partial[None], (count,) + partial.shape)
    return jnp.sum(lax.all_to_all(copies, AXES, 0, 0), axis=0)


def reduced_rows(partial):
    count = lax.axis_size(AXES)
    rows = partial.shape[0]
    share = partial.reshape((count, rows // count) + partial.shape[1:])
    own = jnp.sum(lax.all_to_all(share, AXES, 0, 0), axis=0)
    copies = jnp.broadcast_to(own[None], (count,) + own.shape)
    return lax.all_to_all(copies, AXES, 0, 0).reshape(partial.shape)


def padded_2(cells, sides):
    for axis, dim in sides:
        count = lax.axis_size(axis)
        ends = count - 1
        head = lax.slice_in_dim(cells, 0, 1, axis=dim)
        tail = lax.slice_in_dim(cells, cells.shape[dim] - 1, cells.shape[dim], axis=dim)
        cells = jnp.concatenate(
            [
                lax.ppermute(tail, axis, [(i, (i + 1) % count) for i in range(ends)]),
                cells,
                lax.ppermute(head, axis, [((i + 1) % count, i) for i in range(ends)]),
            ],
            axis=dim,
        )
    return cells


def operate(values, conductance, shift_col):
    padded = padded_2(values, (("wide", 1), ("narrow", 2)))
    center = padded[:, 1:-1, 1:-1, :]
    deeper = jnp.pad(padded, ((0, 0), (0, 0), (0, 0), (1, 1)))
    beside_all = deeper[:, 2:, 1:-1, 1:-1] + deeper[:, :-2, 1:-1, 1:-1]
    beside_all = beside_all + deeper[:, 1:-1, 2:, 1:-1] + deeper[:, 1:-1, :-2, 1:-1]
    beside_all = beside_all + deeper[:, 1:-1, 1:-1, 2:] + deeper[:, 1:-1, 1:-1, :-2]
    return conductance[None] * (6.0 * center - beside_all) + spread(shift_col) * center


def local_dot(left, right):
    return jnp.sum(left * right, axis=(1, 2, 3))


def solve_spread(inputs, conductance, shifts, total_cells):
    shift_col = jnp.repeat(shifts, inputs.shape[0])
    shadow = jnp.tile(inputs, (shifts.shape[0], 1, 1, 1))
    solution = jnp.zeros_like(shadow)
    residual = shadow
    search = shadow
    rho_now = lax.psum(local_dot(shadow, shadow), AXES) / total_cells
    for iteration in range(ITERS):
        search_image = operate(search, conductance, shift_col)
        denominator = lax.psum(local_dot(shadow, search_image), AXES) / total_cells
        step_alpha = rho_now / denominator
        halfway = residual - spread(step_alpha) * search_image
        halfway_image = operate(halfway, conductance, shift_col)
        cross_sum, square_sum, shadow_half, shadow_image = lax.psum(
            (
                local_dot(halfway_image, halfway),
                local_dot(halfway_image, halfway_image),
                local_dot(shadow, halfway),
                local_dot(shadow, halfway_image),
            ),
            AXES,
        )
        step_omega = cross_sum / total_cells / (square_sum / total_cells + 1e-06)
        solution = solution + spread(step_alpha) * search + spread(step_omega) * halfway
        residual = halfway - spread(step_omega) * halfway_image
        rho_next = shadow_half / total_cells - step_omega * (shadow_image / total_cells)
        if iteration + 1 < ITERS:
            step_beta = rho_next / rho_now * (step_alpha / step_omega)
            search = residual + spread(step_beta) * (search - spread(step_omega) * search_image)
            rho_now = rho_next
    return solution.reshape(shadow.shape[0], -1)


def solve_body(shift_ref, field_ref, out_ref, *scratch, dims, slots, total_cells):
    wide, narrow, near, rows = dims
    depth = wide * near // SUB
    height = narrow * rows
    shadow, cond = scratch[0], scratch[1]
    per = scratch[2:]
    names = ("x", "r", "v", "t", "p", "s")
    col = [dict(zip(names, per[6 * a : 6 * a + 6])) for a in range(slots)]
    zero = jnp.zeros((SUB, LANE), jnp.float32)
    lane = lax.broadcasted_iota(jnp.int32, (SUB, LANE), 1)
    sub = lax.broadcasted_iota(jnp.int32, (SUB, LANE), 0)
    first_lane, last_lane = lane == 0, lane == LANE - 1
    first_sub, last_sub = sub == 0, sub == SUB - 1
    jump = depth // near * 2 * near * rows

    for half in range(narrow):
        for i in range(depth):
            for y in range(rows):
                base = (((half * wide + i // near) * 2) * near + i % near) * rows + y
                shadow[i, half * rows + y] = field_ref[pl.ds(base, SUB, stride=jump), :]
                cond[i, half * rows + y] = field_ref[pl.ds(base + near * rows, SUB, stride=jump), :]

    def edges(ref):
        for y in range(height):
            low = pltpu.roll(ref[depth, y + 1], 1, 0)
            ref[0, y + 1] = jnp.where(first_sub, 0.0, low)
            high = pltpu.roll(ref[1, y + 1], SUB - 1, 0)
            ref[depth + 1, y + 1] = jnp.where(last_sub, 0.0, high)

    def image(ref, i, y, here, c, shift):
        nb = ref[i, y + 1] + ref[i + 2, y + 1]
        nb = nb + (ref[i + 1, y] + ref[i + 1, y + 2])
        nb = nb + (
            jnp.where(first_lane, 0.0, pltpu.roll(here, 1, 1)) + jnp.where(last_lane, 0.0, pltpu.roll(here, LANE - 1, 1))
        )
        return c * (6.0 * here - nb) + shift * here

    def mean(acc):
        return jnp.sum(jnp.sum(acc, axis=0, keepdims=True), axis=1, keepdims=True) / total_cells

    def wide_of(scalar):
        return jnp.broadcast_to(scalar, (SUB, LANE))

    for a in range(slots):
        for name in ("p", "s"):
            for i in range(depth + 2):
                col[a][name][i, 0] = zero
                col[a][name][i, height + 1] = zero
    shift = [jnp.full((SUB, LANE), shift_ref[a], jnp.float32) for a in range(slots)]

    def start(i, acc):
        for y in range(height):
            b = shadow[i, y]
            acc = acc + b * b
            for a in range(slots):
                col[a]["p"][i + 1, y + 1] = b
        return acc

    rho0 = wide_of(mean(lax.fori_loop(0, depth, start, zero)))
    rho = [rho0] * slots
    for a in range(slots):
        edges(col[a]["p"])

    for it in range(ITERS):
        first, last = it == 0, it == ITERS - 1

        def phase_a(i, acc):
            acc = list(acc)
            for y in range(height):
                b, c = shadow[i, y], cond[i, y]
                for a in range(slots):
                    p = col[a]["p"]
                    v = image(p, i, y, p[i + 1, y + 1], c, shift[a])
                    col[a]["v"][i, y] = v
                    acc[a] = acc[a] + b * v
            return tuple(acc)

        acc = lax.fori_loop(0, depth, phase_a, (zero,) * slots)
        alpha = [rho[a] / wide_of(mean(acc[a])) for a in range(slots)]

        def phase_b(i, _):
            for y in range(height):
                for a in range(slots):
                    r = shadow[i, y] if first else col[a]["r"][i, y]
                    col[a]["s"][i + 1, y + 1] = r - alpha[a] * col[a]["v"][i, y]
            return 0

        lax.fori_loop(0, depth, phase_b, 0)
        for a in range(slots):
            edges(col[a]["s"])

        def phase_c(i, acc):
            acc = [list(one) for one in acc]
            for y in range(height):
                b, c = shadow[i, y], cond[i, y]
                for a in range(slots):
                    ref = col[a]["s"]
                    s = ref[i + 1, y + 1]
                    t = image(ref, i, y, s, c, shift[a])
                    col[a]["t"][i, y] = t
                    acc[a][0] = acc[a][0] + t * s
                    acc[a][1] = acc[a][1] + t * t
                    if not last:
                        acc[a][2] = acc[a][2] + b * s
                        acc[a][3] = acc[a][3] + b * t
            return tuple(tuple(one) for one in acc)

        acc = lax.fori_loop(0, depth, phase_c, ((zero,) * (2 if last else 4),) * slots)
        omega, beta = [], []
        for a in range(slots):
            means = [wide_of(mean(one)) for one in acc[a]]
            omega.append(means[0] / (means[1] + 1e-06))
            if not last:
                rho_next = means[2] - omega[a] * means[3]
                beta.append(rho_next / rho[a] * (alpha[a] / omega[a]))
                rho[a] = rho_next

        def phase_d(i, _):
            for y in range(height):
                for a in range(slots):
                    p, s = col[a]["p"][i + 1, y + 1], col[a]["s"][i + 1, y + 1]
                    x = alpha[a] * p + omega[a] * s
                    if not first:
                        x = col[a]["x"][i, y] + x
                    col[a]["x"][i, y] = x
                    if not last:
                        r = s - omega[a] * col[a]["t"][i, y]
                        col[a]["r"][i, y] = r
                        col[a]["p"][i + 1, y + 1] = r + beta[a] * (p - omega[a] * col[a]["v"][i, y])
            return 0

        lax.fori_loop(0, depth, phase_d, 0)
        if not last:
            for a in range(slots):
                edges(col[a]["p"])

    for half in range(narrow):
        for a in range(slots):
            for i in range(depth):
                for y in range(rows):
                    base = ((half * slots + a) * depth * SUB + i) * rows + y
                    out_ref[pl.ds(base, SUB, stride=depth * rows), :] = col[a]["x"][i, half * rows + y]


def solve_whole(inputs, conductance, shifts, total_cells):
    wide, narrow = lax.axis_size("wide"), lax.axis_size("narrow")
    columns, near, rows, lanes = inputs.shape
    count = shifts.shape[0]
    slots = -(-count // narrow)
    sent = jnp.stack([inputs, jnp.broadcast_to(conductance[None], inputs.shape)], axis=1)
    got = lax.all_to_all(sent, "wide", 0, 0)
    fields = lax.all_gather(got, "narrow", axis=0)
    mine = lax.axis_index("narrow") * slots + jnp.arange(slots)
    own_shifts = shifts[jnp.minimum(mine, count - 1)]
    planes, height = wide * near, narrow * rows
    depth = planes // SUB
    plain = pltpu.VMEM((depth, height, SUB, LANE), jnp.float32)
    ringed = pltpu.VMEM((depth + 2, height + 2, SUB, LANE), jnp.float32)
    x = pl.pallas_call(
        functools.partial(solve_body, dims=(wide, narrow, near, rows), slots=slots, total_cells=total_cells),
        out_shape=jax.ShapeDtypeStruct((narrow * slots * planes * rows, LANE), jnp.float32),
        in_specs=[pl.BlockSpec(memory_space=pltpu.SMEM), pl.BlockSpec(memory_space=pltpu.VMEM)],
        out_specs=pl.BlockSpec(memory_space=pltpu.VMEM),
        scratch_shapes=[plain, plain] + [plain, plain, plain, plain, ringed, ringed] * slots,
        name="solve_whole",
    )(own_shifts, fields.reshape(-1, LANE))
    x = x.reshape(narrow, slots, wide, near * rows * lanes)
    x = lax.all_to_all(x, "narrow", 0, 0)
    x = x.reshape(narrow * slots, wide, -1)[:count]
    return lax.all_to_all(x.transpose(1, 0, 2), "wide", 0, 0)


def fits_whole(inputs, shifts):
    wide, narrow = lax.axis_size("wide"), lax.axis_size("narrow")
    columns, near, rows, lanes = inputs.shape
    slots = -(-shifts.shape[0] // narrow)
    field = wide * narrow * near * rows * lanes * 4
    return (
        columns == wide
        and lanes == LANE
        and wide % SUB == 0
        and rows % SUB == 0
        and field * (8 + 8 * slots) <= 24 * 2**20
    )


def shards(inputs, old_basis, conductance, shifts):
    total_cells = math.prod(inputs.shape[1:]) * lax.axis_size(AXES)
    columns, count = inputs.shape[0], shifts.shape[0]
    vflat = old_basis.reshape(old_basis.shape[0], -1)
    high = lax.Precision.HIGHEST
    gram = jnp.einsum("bc,dc->bd", vflat, vflat, precision=high)
    whole = fits_whole(inputs, shifts)
    if whole:
        wflat = solve_whole(inputs, conductance, shifts, total_cells).reshape(columns * count, -1)
    else:
        wflat = solve_spread(inputs, conductance, shifts, total_cells)
    first = jnp.einsum("bc,kc->bk", vflat, wflat, precision=high)
    if old_basis.shape[0] % lax.axis_size(AXES) == 0:
        both = reduced_rows(jnp.concatenate([first, gram], axis=1))
    else:
        both = lax.psum(jnp.concatenate([first, gram], axis=1), AXES)
    both = both / total_cells
    first, gram = both[:, : columns * count], both[:, columns * count :]
    coef = first + (first - jnp.matmul(gram, first, precision=high))
    twice = wflat - jnp.einsum("bk,bc->kc", coef, vflat, precision=high)
    mean_square = reduced(jnp.sum(twice * twice, axis=1)) / total_cells
    col_scale = jnp.sqrt(mean_square + 1e-06)
    new_columns = twice / col_scale[:, None]
    if whole:
        new_columns = new_columns.reshape(columns, count, -1).transpose(1, 0, 2)
        coef = coef.reshape(-1, columns, count).transpose(0, 2, 1).reshape(-1, columns * count)
        col_scale = col_scale.reshape(columns, count).T.reshape(-1)
    return (new_columns.reshape((columns * count,) + inputs.shape[1:]), coef, col_scale)


def solution(mesh):
    in_specs = (
        P(None, "wide", "narrow", None),
        P(None, "wide", "narrow", None),
        P("wide", "narrow", None),
        P(),
    )
    out_specs = (P(None, "wide", "narrow", None), P(), P())
    return jax.shard_map(shards, mesh=mesh, in_specs=in_specs, out_specs=out_specs, check_vma=False)
```

```python
import functools
import math

import jax
import jax.numpy as jnp
from jax import lax
from jax.experimental import pallas as pl
from jax.experimental.pallas import tpu as pltpu
from jax.sharding import PartitionSpec as P

ITERS = 4
AXES = ("wide", "narrow")
SUB, LANE = 8, 128


def spread(coef):
    return coef[:, None, None, None]


def reduced(partial):
    count = lax.axis_size(AXES)
    copies = jnp.broadcast_to(partial[None], (count,) + partial.shape)
    return jnp.sum(lax.all_to_all(copies, AXES, 0, 0), axis=0)


def reduced_rows(partial):
    count = lax.axis_size(AXES)
    rows = partial.shape[0]
    share = partial.reshape((count, rows // count) + partial.shape[1:])
    own = jnp.sum(lax.all_to_all(share, AXES, 0, 0), axis=0)
    copies = jnp.broadcast_to(own[None], (count,) + own.shape)
    return lax.all_to_all(copies, AXES, 0, 0).reshape(partial.shape)


def padded_2(cells, sides):
    for axis, dim in sides:
        count = lax.axis_size(axis)
        ends = count - 1
        head = lax.slice_in_dim(cells, 0, 1, axis=dim)
        tail = lax.slice_in_dim(cells, cells.shape[dim] - 1, cells.shape[dim], axis=dim)
        cells = jnp.concatenate(
            [
                lax.ppermute(tail, axis, [(i, (i + 1) % count) for i in range(ends)]),
                cells,
                lax.ppermute(head, axis, [((i + 1) % count, i) for i in range(ends)]),
            ],
            axis=dim,
        )
    return cells


def operate(values, conductance, shift_col):
    padded = padded_2(values, (("wide", 1), ("narrow", 2)))
    center = padded[:, 1:-1, 1:-1, :]
    deeper = jnp.pad(padded, ((0, 0), (0, 0), (0, 0), (1, 1)))
    beside_all = deeper[:, 2:, 1:-1, 1:-1] + deeper[:, :-2, 1:-1, 1:-1]
    beside_all = beside_all + deeper[:, 1:-1, 2:, 1:-1] + deeper[:, 1:-1, :-2, 1:-1]
    beside_all = beside_all + deeper[:, 1:-1, 1:-1, 2:] + deeper[:, 1:-1, 1:-1, :-2]
    return conductance[None] * (6.0 * center - beside_all) + spread(shift_col) * center


def local_dot(left, right):
    return jnp.sum(left * right, axis=(1, 2, 3))


def solve_spread(inputs, conductance, shifts, total_cells):
    shift_col = jnp.repeat(shifts, inputs.shape[0])
    shadow = jnp.tile(inputs, (shifts.shape[0], 1, 1, 1))
    solution = jnp.zeros_like(shadow)
    residual = shadow
    search = shadow
    rho_now = lax.psum(local_dot(shadow, shadow), AXES) / total_cells
    for iteration in range(ITERS):
        search_image = operate(search, conductance, shift_col)
        denominator = lax.psum(local_dot(shadow, search_image), AXES) / total_cells
        step_alpha = rho_now / denominator
        halfway = residual - spread(step_alpha) * search_image
        halfway_image = operate(halfway, conductance, shift_col)
        cross_sum, square_sum, shadow_half, shadow_image = lax.psum(
            (
                local_dot(halfway_image, halfway),
                local_dot(halfway_image, halfway_image),
                local_dot(shadow, halfway),
                local_dot(shadow, halfway_image),
            ),
            AXES,
        )
        step_omega = cross_sum / total_cells / (square_sum / total_cells + 1e-06)
        solution = solution + spread(step_alpha) * search + spread(step_omega) * halfway
        residual = halfway - spread(step_omega) * halfway_image
        rho_next = shadow_half / total_cells - step_omega * (shadow_image / total_cells)
        if iteration + 1 < ITERS:
            step_beta = rho_next / rho_now * (step_alpha / step_omega)
            search = residual + spread(step_beta) * (search - spread(step_omega) * search_image)
            rho_now = rho_next
    return solution.reshape(shadow.shape[0], -1)


def split_columns(count, narrow):
    return count // narrow, count % narrow


def solve_body(core_ref, shift_ref, *refs, dims, count, total_cells):
    wide, narrow, near, rows = dims
    own, left = split_columns(count, narrow)
    slots = own + left
    depth = wide * near // SUB
    height = narrow * rows
    parts, out_ref, (shadow, cond), per = refs[:narrow], refs[narrow], refs[narrow + 1 : narrow + 3], refs[narrow + 3 :]
    names = ("x", "r", "v", "t", "p", "s")
    col = [dict(zip(names, per[6 * a : 6 * a + 6])) for a in range(slots)]
    core = core_ref[0]
    zero = jnp.zeros((SUB, LANE), jnp.float32)
    lane = lax.broadcasted_iota(jnp.int32, (SUB, LANE), 1)
    sub = lax.broadcasted_iota(jnp.int32, (SUB, LANE), 0)
    first_lane, last_lane = lane == 0, lane == LANE - 1
    first_sub, last_sub = sub == 0, sub == SUB - 1
    apart = depth // near

    for step in range(narrow):
        at = lax.rem(core + step, narrow) * rows
        for i in range(depth):
            for y in range(rows):
                base = ((i // near * 2) * near + i % near) * rows + y
                jump = apart * 2 * near * rows
                shadow[i, at + y] = parts[step][pl.ds(base, SUB, stride=jump), :]
                cond[i, at + y] = parts[step][pl.ds(base + near * rows, SUB, stride=jump), :]

    def edges(ref):
        for y in range(height):
            low = pltpu.roll(ref[depth, y + 1], 1, 0)
            ref[0, y + 1] = jnp.where(first_sub, 0.0, low)
            high = pltpu.roll(ref[1, y + 1], SUB - 1, 0)
            ref[depth + 1, y + 1] = jnp.where(last_sub, 0.0, high)

    def image(ref, i, y, here, c, shift):
        nb = ref[i, y + 1] + ref[i + 2, y + 1]
        nb = nb + (ref[i + 1, y] + ref[i + 1, y + 2])
        nb = nb + (
            jnp.where(first_lane, 0.0, pltpu.roll(here, 1, 1)) + jnp.where(last_lane, 0.0, pltpu.roll(here, LANE - 1, 1))
        )
        return c * (6.0 * here - nb) + shift * here

    def mean(acc):
        return jnp.sum(jnp.sum(acc, axis=0, keepdims=True), axis=1, keepdims=True) / total_cells

    def wide_of(scalar):
        return jnp.broadcast_to(scalar, (SUB, LANE))

    for a in range(slots):
        for name in ("p", "s"):
            for i in range(depth + 2):
                col[a][name][i, 0] = zero
                col[a][name][i, height + 1] = zero
    which = [core * own + a for a in range(own)] + [narrow * own + a for a in range(left)]
    shift = [jnp.full((SUB, LANE), shift_ref[j], jnp.float32) for j in which]

    def start(i, acc):
        for y in range(height):
            b = shadow[i, y]
            acc = acc + b * b
            for a in range(slots):
                col[a]["p"][i + 1, y + 1] = b
        return acc

    rho0 = wide_of(mean(lax.fori_loop(0, depth, start, zero)))
    rho = [rho0] * slots
    for a in range(slots):
        edges(col[a]["p"])

    for it in range(ITERS):
        first, last = it == 0, it == ITERS - 1

        def phase_a(i, acc):
            acc = list(acc)
            for y in range(height):
                b, c = shadow[i, y], cond[i, y]
                for a in range(slots):
                    p = col[a]["p"]
                    v = image(p, i, y, p[i + 1, y + 1], c, shift[a])
                    col[a]["v"][i, y] = v
                    acc[a] = acc[a] + b * v
            return tuple(acc)

        acc = lax.fori_loop(0, depth, phase_a, (zero,) * slots)
        alpha = [rho[a] / wide_of(mean(acc[a])) for a in range(slots)]

        def phase_b(i, _):
            for y in range(height):
                for a in range(slots):
                    r = shadow[i, y] if first else col[a]["r"][i, y]
                    col[a]["s"][i + 1, y + 1] = r - alpha[a] * col[a]["v"][i, y]
            return 0

        lax.fori_loop(0, depth, phase_b, 0)
        for a in range(slots):
            edges(col[a]["s"])

        def phase_c(i, acc):
            acc = [list(one) for one in acc]
            for y in range(height):
                b, c = shadow[i, y], cond[i, y]
                for a in range(slots):
                    ref = col[a]["s"]
                    s = ref[i + 1, y + 1]
                    t = image(ref, i, y, s, c, shift[a])
                    col[a]["t"][i, y] = t
                    acc[a][0] = acc[a][0] + t * s
                    acc[a][1] = acc[a][1] + t * t
                    if not last:
                        acc[a][2] = acc[a][2] + b * s
                        acc[a][3] = acc[a][3] + b * t
            return tuple(tuple(one) for one in acc)

        acc = lax.fori_loop(0, depth, phase_c, ((zero,) * (2 if last else 4),) * slots)
        omega, beta = [], []
        for a in range(slots):
            means = [wide_of(mean(one)) for one in acc[a]]
            omega.append(means[0] / (means[1] + 1e-06))
            if not last:
                rho_next = means[2] - omega[a] * means[3]
                beta.append(rho_next / rho[a] * (alpha[a] / omega[a]))
                rho[a] = rho_next

        def phase_d(i, _):
            for y in range(height):
                for a in range(slots):
                    p, s = col[a]["p"][i + 1, y + 1], col[a]["s"][i + 1, y + 1]
                    x = alpha[a] * p + omega[a] * s
                    if not first:
                        x = col[a]["x"][i, y] + x
                    col[a]["x"][i, y] = x
                    if not last:
                        r = s - omega[a] * col[a]["t"][i, y]
                        col[a]["r"][i, y] = r
                        col[a]["p"][i + 1, y + 1] = r + beta[a] * (p - omega[a] * col[a]["v"][i, y])
            return 0

        lax.fori_loop(0, depth, phase_d, 0)
        if not last:
            for a in range(slots):
                edges(col[a]["p"])

    share = near // narrow
    chunk = own * near + left * share
    jump = apart * narrow * chunk * rows
    for to in range(narrow):
        for group in range(apart):
            for y in range(rows):
                base = ((group * narrow + to) * chunk) * rows + y
                for a in range(own):
                    for xl in range(near):
                        at = base + (a * near + xl) * rows
                        out_ref[pl.ds(at, SUB, stride=jump), :] = col[a]["x"][group * near + xl, to * rows + y]
                for e in range(left):
                    for xl in range(share):
                        at = base + (own * near + e * share + xl) * rows
                        from_i = group * near + core * share + xl
                        out_ref[pl.ds(at, SUB, stride=jump), :] = col[own + e]["x"][from_i, to * rows + y]


def solve_whole(inputs, conductance, shifts, total_cells):
    wide, narrow = lax.axis_size("wide"), lax.axis_size("narrow")
    columns, near, rows, lanes = inputs.shape
    count = shifts.shape[0]
    own, left = split_columns(count, narrow)
    slots = own + left
    sent = jnp.stack([inputs, jnp.broadcast_to(conductance[None], inputs.shape)], axis=1)
    got = lax.all_to_all(sent, "wide", 0, 0).reshape(-1, LANE)
    parts = [got]
    for step in range(1, narrow):
        parts.append(lax.ppermute(got, "narrow", [((i + step) % narrow, i) for i in range(narrow)]))
    planes, height = wide * near, narrow * rows
    depth = planes // SUB
    plain = pltpu.VMEM((depth, height, SUB, LANE), jnp.float32)
    ringed = pltpu.VMEM((depth + 2, height + 2, SUB, LANE), jnp.float32)
    share = near // narrow
    chunk = own * near + left * share
    smem, vmem = pl.BlockSpec(memory_space=pltpu.SMEM), pl.BlockSpec(memory_space=pltpu.VMEM)
    x = pl.pallas_call(
        functools.partial(solve_body, dims=(wide, narrow, near, rows), count=count, total_cells=total_cells),
        out_shape=jax.ShapeDtypeStruct((wide * narrow * chunk * rows, LANE), jnp.float32),
        in_specs=[smem, smem] + [vmem] * narrow,
        out_specs=vmem,
        scratch_shapes=[plain, plain] + [plain, plain, plain, plain, ringed, ringed] * slots,
        name="solve_whole",
    )(lax.axis_index("narrow").reshape(1), shifts, *parts)
    x = lax.all_to_all(x.reshape(wide * narrow, chunk, rows, LANE), AXES, 0, 0)
    x = x.reshape(wide, narrow, chunk, rows * lanes)
    full = x[:, :, : own * near].reshape(wide, narrow * own, near * rows * lanes)
    rest = x[:, :, own * near :].reshape(wide, narrow, left, share, rows * lanes).transpose(0, 2, 1, 3, 4)
    return jnp.concatenate([full, rest.reshape(wide, left, near * rows * lanes)], axis=1)


def fits_whole(inputs, shifts):
    wide, narrow = lax.axis_size("wide"), lax.axis_size("narrow")
    columns, near, rows, lanes = inputs.shape
    own, left = split_columns(shifts.shape[0], narrow)
    field = wide * narrow * near * rows * lanes * 4
    return (
        columns == wide
        and lanes == LANE
        and wide % SUB == 0
        and rows % SUB == 0
        and near % narrow == 0
        and field * (6 + 8 * (own + left)) <= 24 * 2**20
    )


def shards(inputs, old_basis, conductance, shifts):
    total_cells = math.prod(inputs.shape[1:]) * lax.axis_size(AXES)
    columns, count = inputs.shape[0], shifts.shape[0]
    width, basis = columns * count, old_basis.shape[0]
    vflat = old_basis.reshape(basis, -1)
    high = lax.Precision.HIGHEST
    gram = jnp.einsum("bc,dc->bd", vflat, vflat, precision=high)
    whole = fits_whole(inputs, shifts)
    if whole:
        wflat = solve_whole(inputs, conductance, shifts, total_cells).reshape(width, -1)
    else:
        wflat = solve_spread(inputs, conductance, shifts, total_cells)
    first = jnp.einsum("bc,kc->bk", vflat, wflat, precision=high)
    square = jnp.sum(wflat * wflat, axis=1)
    tall = max(basis, width)
    square = jnp.pad(square, (0, tall - width))[:, None]
    both = jnp.concatenate([jnp.pad(jnp.concatenate([first, gram], axis=1), ((0, tall - basis), (0, 0))), square], axis=1)
    if tall % lax.axis_size(AXES) == 0:
        both = reduced_rows(both)
    else:
        both = lax.psum(both, AXES)
    both = both / total_cells
    first, gram, square = both[:basis, :width], both[:basis, width:-1], both[:width, -1]
    coef = first + (first - jnp.matmul(gram, first, precision=high))
    twice = wflat - jnp.einsum("bk,bc->kc", coef, vflat, precision=high)
    crossed = 2.0 * jnp.sum(coef * first, axis=0)
    folded = jnp.sum(coef * jnp.matmul(gram, coef, precision=high), axis=0)
    quick = square - crossed + folded
    safe = jnp.all(quick >= 0.1 * (square + jnp.abs(crossed) + folded))
    mean_square = lax.cond(safe, lambda: quick, lambda: reduced(jnp.sum(twice * twice, axis=1)) / total_cells)
    col_scale = jnp.sqrt(mean_square + 1e-06)
    new_columns = twice / col_scale[:, None]
    if whole:
        new_columns = new_columns.reshape(columns, count, -1).transpose(1, 0, 2)
        coef = coef.reshape(-1, columns, count).transpose(0, 2, 1).reshape(-1, width)
        col_scale = col_scale.reshape(columns, count).T.reshape(-1)
    return (new_columns.reshape((width,) + inputs.shape[1:]), coef, col_scale)


def solution(mesh):
    in_specs = (
        P(None, "wide", "narrow", None),
        P(None, "wide", "narrow", None),
        P("wide", "narrow", None),
        P(),
    )
    out_specs = (P(None, "wide", "narrow", None), P(), P())
    return jax.shard_map(shards, mesh=mesh, in_specs=in_specs, out_specs=out_specs, check_vma=False)
```

```python
import functools
import math

import jax
import jax.numpy as jnp
from jax import lax
from jax.experimental import pallas as pl
from jax.experimental.pallas import tpu as pltpu
from jax.sharding import PartitionSpec as P

ITERS = 4
AXES = ("wide", "narrow")
SUB, LANE = 8, 128
UNROLL = 64


def spread(coef):
    return coef[:, None, None, None]


def reduced(partial):
    count = lax.axis_size(AXES)
    copies = jnp.broadcast_to(partial[None], (count,) + partial.shape)
    return jnp.sum(lax.all_to_all(copies, AXES, 0, 0), axis=0)


def reduced_rows(partial):
    count = lax.axis_size(AXES)
    share = partial.reshape((count, partial.shape[0] // count) + partial.shape[1:])
    own = jnp.sum(lax.all_to_all(share, AXES, 0, 0), axis=0)
    copies = jnp.broadcast_to(own[None], (count,) + own.shape)
    return lax.all_to_all(copies, AXES, 0, 0).reshape(partial.shape)


def padded_2(cells, sides):
    for axis, dim in sides:
        count = lax.axis_size(axis)
        ends = count - 1
        head = lax.slice_in_dim(cells, 0, 1, axis=dim)
        tail = lax.slice_in_dim(cells, cells.shape[dim] - 1, cells.shape[dim], axis=dim)
        cells = jnp.concatenate(
            [
                lax.ppermute(tail, axis, [(i, (i + 1) % count) for i in range(ends)]),
                cells,
                lax.ppermute(head, axis, [((i + 1) % count, i) for i in range(ends)]),
            ],
            axis=dim,
        )
    return cells


def operate(values, conductance, shift_col):
    padded = padded_2(values, (("wide", 1), ("narrow", 2)))
    center = padded[:, 1:-1, 1:-1, :]
    deeper = jnp.pad(padded, ((0, 0), (0, 0), (0, 0), (1, 1)))
    beside_all = deeper[:, 2:, 1:-1, 1:-1] + deeper[:, :-2, 1:-1, 1:-1]
    beside_all = beside_all + deeper[:, 1:-1, 2:, 1:-1] + deeper[:, 1:-1, :-2, 1:-1]
    beside_all = beside_all + deeper[:, 1:-1, 1:-1, 2:] + deeper[:, 1:-1, 1:-1, :-2]
    return conductance[None] * (6.0 * center - beside_all) + spread(shift_col) * center


def local_dot(left, right):
    return jnp.sum(left * right, axis=(1, 2, 3))


def solve_spread(inputs, conductance, shifts, total_cells):
    shift_col = jnp.repeat(shifts, inputs.shape[0])
    shadow = jnp.tile(inputs, (shifts.shape[0], 1, 1, 1))
    solution = jnp.zeros_like(shadow)
    residual = shadow
    search = shadow
    rho_now = lax.psum(local_dot(shadow, shadow), AXES) / total_cells
    for iteration in range(ITERS):
        search_image = operate(search, conductance, shift_col)
        denominator = lax.psum(local_dot(shadow, search_image), AXES) / total_cells
        step_alpha = rho_now / denominator
        halfway = residual - spread(step_alpha) * search_image
        halfway_image = operate(halfway, conductance, shift_col)
        cross_sum, square_sum, shadow_half, shadow_image = lax.psum(
            (
                local_dot(halfway_image, halfway),
                local_dot(halfway_image, halfway_image),
                local_dot(shadow, halfway),
                local_dot(shadow, halfway_image),
            ),
            AXES,
        )
        step_omega = cross_sum / total_cells / (square_sum / total_cells + 1e-06)
        solution = solution + spread(step_alpha) * search + spread(step_omega) * halfway
        residual = halfway - spread(step_omega) * halfway_image
        rho_next = shadow_half / total_cells - step_omega * (shadow_image / total_cells)
        if iteration + 1 < ITERS:
            step_beta = rho_next / rho_now * (step_alpha / step_omega)
            search = residual + spread(step_beta) * (search - spread(step_omega) * search_image)
            rho_now = rho_next
    return solution.reshape(shadow.shape[0], -1)


def split_columns(count, narrow):
    return count // narrow, count % narrow


def solve_body(core_ref, shift_ref, *refs, dims, count, total_cells):
    wide, narrow, near, rows = dims
    own, left = split_columns(count, narrow)
    slots = own + left
    planes, height = wide * near, narrow * rows
    parts, out_ref, (shadow, cond), per = refs[:narrow], refs[narrow], refs[narrow + 1 : narrow + 3], refs[narrow + 3 :]
    names = ("x", "r", "v", "t", "p", "s")
    col = [dict(zip(names, per[6 * a : 6 * a + 6])) for a in range(slots)]
    core = core_ref[0]
    zero = jnp.zeros((SUB, LANE), jnp.float32)
    lane = lax.broadcasted_iota(jnp.int32, (SUB, LANE), 1)
    first_lane, last_lane = lane == 0, lane == LANE - 1
    group = UNROLL
    tiles = range(0, height, SUB)

    for step in range(narrow):
        at = pl.multiple_of(lax.rem(core + step, narrow) * rows, SUB)
        shadow_half, cond_half = shadow.at[:, pl.ds(at, rows)], cond.at[:, pl.ds(at, rows)]
        for w in range(wide):
            shadow_half[w * near : (w + 1) * near] = parts[step][w, 0]
            cond_half[w * near : (w + 1) * near] = parts[step][w, 1]

    def clear(i, _):
        for a in range(slots):
            for name in ("p", "s"):
                col[a][name][i, :SUB, :] = zero
                col[a][name][i, SUB + height :, :] = zero
        return 0

    lax.fori_loop(0, planes + 2, clear, 0)
    for a in range(slots):
        for name in ("p", "s"):
            for i in (0, planes + 1):
                for y in tiles:
                    col[a][name][i, SUB + y : 2 * SUB + y, :] = zero

    def inner(ref, i, y):
        return ref[i + 1, SUB + y : 2 * SUB + y, :]

    def image(ref, i, y, here, c, shift):
        nb = ref[i, SUB + y : 2 * SUB + y, :] + ref[i + 2, SUB + y : 2 * SUB + y, :]
        nb = nb + (ref[i + 1, SUB + y - 1 : 2 * SUB + y - 1, :] + ref[i + 1, SUB + y + 1 : 2 * SUB + y + 1, :])
        nb = nb + (
            jnp.where(first_lane, 0.0, pltpu.roll(here, 1, 1)) + jnp.where(last_lane, 0.0, pltpu.roll(here, LANE - 1, 1))
        )
        return c * (6.0 * here - nb) + shift * here

    def mean(acc):
        total = jnp.sum(jnp.sum(acc, axis=1, keepdims=True), axis=0, keepdims=True) / total_cells
        return jnp.broadcast_to(total, (SUB, LANE))

    def over(body, carry):
        def some(g, carry):
            for u in range(group):
                for y in tiles:
                    carry = body(g * group + u, y, carry)
            return carry

        return lax.fori_loop(0, planes // group, some, carry)

    which = [core * own + a for a in range(own)] + [narrow * own + a for a in range(left)]
    shift = [jnp.full((SUB, LANE), shift_ref[j], jnp.float32) for j in which]

    def at_tile(ref, i, y):
        return ref[i, y : y + SUB, :]

    def start(i, y, acc):
        b = at_tile(shadow, i, y)
        for a in range(slots):
            col[a]["p"][i + 1, SUB + y : 2 * SUB + y, :] = b
            col[a]["r"][i, y : y + SUB, :] = b
            col[a]["x"][i, y : y + SUB, :] = zero
        return acc + b * b

    def half_step(rho, last):
        def phase_a(i, y, acc):
            b, c = at_tile(shadow, i, y), at_tile(cond, i, y)
            out = []
            for a in range(slots):
                p = col[a]["p"]
                v = image(p, i, y, inner(p, i, y), c, shift[a])
                col[a]["v"][i, y : y + SUB, :] = v
                out.append(acc[a] + b * v)
            return tuple(out)

        acc = over(phase_a, (zero,) * slots)
        alpha = [rho[a] / mean(acc[a]) for a in range(slots)]

        def phase_b(i, y, _):
            for a in range(slots):
                s = at_tile(col[a]["r"], i, y) - alpha[a] * at_tile(col[a]["v"], i, y)
                col[a]["s"][i + 1, SUB + y : 2 * SUB + y, :] = s
            return 0

        over(phase_b, 0)

        def phase_c(i, y, acc):
            b, c = at_tile(shadow, i, y), at_tile(cond, i, y)
            out = []
            for a in range(slots):
                ref = col[a]["s"]
                s = inner(ref, i, y)
                t = image(ref, i, y, s, c, shift[a])
                one = [acc[a][0] + t * s, acc[a][1] + t * t]
                if not last:
                    col[a]["t"][i, y : y + SUB, :] = t
                    one += [acc[a][2] + b * s, acc[a][3] + b * t]
                out.append(tuple(one))
            return tuple(out)

        acc = over(phase_c, ((zero,) * (2 if last else 4),) * slots)
        means = [[mean(one) for one in acc[a]] for a in range(slots)]
        omega = [m[0] / (m[1] + 1e-06) for m in means]
        return alpha, omega, means

    def full_step(_, rho):
        alpha, omega, means = half_step(rho, False)
        rho_next = [means[a][2] - omega[a] * means[a][3] for a in range(slots)]
        beta = [rho_next[a] / rho[a] * (alpha[a] / omega[a]) for a in range(slots)]

        def phase_d(i, y, _):
            for a in range(slots):
                p, s = inner(col[a]["p"], i, y), inner(col[a]["s"], i, y)
                col[a]["x"][i, y : y + SUB, :] = at_tile(col[a]["x"], i, y) + (alpha[a] * p + omega[a] * s)
                r = s - omega[a] * at_tile(col[a]["t"], i, y)
                col[a]["r"][i, y : y + SUB, :] = r
                next_p = r + beta[a] * (p - omega[a] * at_tile(col[a]["v"], i, y))
                col[a]["p"][i + 1, SUB + y : 2 * SUB + y, :] = next_p
            return 0

        over(phase_d, 0)
        return tuple(rho_next)

    rho0 = mean(over(start, zero))
    rho = lax.fori_loop(0, ITERS - 1, full_step, (rho0,) * slots)
    alpha, omega, _ = half_step(rho, True)

    share = near // narrow
    chunk = own * near + left * share

    def finished(a, i, y):
        p, s = inner(col[a]["p"], i, y), inner(col[a]["s"], i, y)
        return at_tile(col[a]["x"], i, y) + (alpha[a] * p + omega[a] * s)

    def send(w, _):
        for to in range(narrow):
            base = (w * narrow + to) * chunk
            for a in range(own):
                for xl in range(near):
                    out_ref[base + a * near + xl] = finished(a, w * near + xl, to * rows)
            for e in range(left):
                for xl in range(share):
                    i = w * near + core * share + xl
                    out_ref[base + own * near + e * share + xl] = finished(own + e, i, to * rows)
        return 0

    lax.fori_loop(0, wide, send, 0)


def solve_whole(inputs, conductance, shifts, total_cells, beside):
    wide, narrow = lax.axis_size("wide"), lax.axis_size("narrow")
    columns, near, rows, lanes = inputs.shape
    count = shifts.shape[0]
    own, left = split_columns(count, narrow)
    slots = own + left
    sent = jnp.stack([inputs, jnp.broadcast_to(conductance[None], inputs.shape)], axis=1)
    got = lax.all_to_all(sent, "wide", 0, 0)
    got, beside = lax.optimization_barrier((got, beside))
    parts = [got]
    for step in range(1, narrow):
        parts.append(lax.ppermute(got, "narrow", [((i + step) % narrow, i) for i in range(narrow)]))
    planes, height = wide * near, narrow * rows
    plain = pltpu.VMEM((planes, height, LANE), jnp.float32)
    ringed = pltpu.VMEM((planes + 2, height + 2 * SUB, LANE), jnp.float32)
    share = near // narrow
    chunk = own * near + left * share
    smem, vmem = pl.BlockSpec(memory_space=pltpu.SMEM), pl.BlockSpec(memory_space=pltpu.VMEM)
    x = pl.pallas_call(
        functools.partial(solve_body, dims=(wide, narrow, near, rows), count=count, total_cells=total_cells),
        out_shape=jax.ShapeDtypeStruct((wide * narrow * chunk, rows, LANE), jnp.float32),
        in_specs=[smem, smem] + [vmem] * narrow,
        out_specs=vmem,
        scratch_shapes=[plain, plain] + [plain, plain, plain, plain, ringed, ringed] * slots,
        name="solve_whole",
    )(lax.axis_index("narrow").reshape(1), shifts, *parts)
    return lax.all_to_all(x.reshape(wide * narrow, chunk, rows, LANE), AXES, 0, 0), beside


def terms(value):
    high = value.astype(jnp.bfloat16)
    rest = value - high.astype(jnp.float32)
    mid = rest.astype(jnp.bfloat16)
    return high, mid, (rest - mid.astype(jnp.float32)).astype(jnp.bfloat16)


def basis_body(source, *parts, group, held):
    for r in range(held):
        for g in range(0, group, 2 * SUB):
            low = source[pl.ds(g * held + r, SUB, stride=held), :]
            high = source[pl.ds((g + SUB) * held + r, SUB, stride=held), :]
            for part, value in zip(parts, terms(jnp.concatenate([low, high], axis=0))):
                part[g : g + 2 * SUB, r * LANE : (r + 1) * LANE] = value


def basis_terms(old_basis):
    basis = old_basis.shape[0]
    held = old_basis.shape[1] * old_basis.shape[2]
    group = 2 * SUB
    out = jax.ShapeDtypeStruct((basis, held * LANE), jnp.bfloat16)
    return pl.pallas_call(
        functools.partial(basis_body, group=group, held=held),
        grid=(basis // group,),
        out_shape=(out,) * 3,
        in_specs=[pl.BlockSpec((group * held, LANE), lambda g: (g, 0))],
        out_specs=(pl.BlockSpec((group, held * LANE), lambda g: (g, 0)),) * 3,
        name="basis_terms",
    )(old_basis.reshape(-1, LANE))


def column_row(j, xl, y, dims, count):
    wide, narrow, near, rows = dims
    own, left = split_columns(count, narrow)
    share = near // narrow
    chunk = own * near + left * share
    if j < narrow * own:
        plane = (j // own) * chunk + (j % own) * near + xl
    else:
        plane = (xl // share) * chunk + own * near + (j - narrow * own) * share + xl % share
    return plane * rows + y, narrow * chunk * rows


def layout_rows(width, basis, devices):
    blocks = basis // LANE
    used = width * blocks + LANE * blocks * (blocks + 1) // 2 + SUB
    step = devices * SUB
    return -(-used // step) * step


def block_row(width, blocks, p, q):
    return width * blocks + LANE * (p * blocks - p * (p - 1) // 2 + q - p)


def first_body(x_ref, gram, high, mid, low, out_ref, x_terms, totals, squares, *, dims, count):
    wide, narrow, near, rows = dims
    width = wide * count
    basis = high.shape[0]
    blocks = basis // LANE
    xl = pl.program_id(0)

    @pl.when(xl == 0)
    def _():
        totals[...] = jnp.zeros_like(totals)
        squares[...] = jnp.zeros_like(squares)

    for j in range(count):
        for w in range(0, wide, 2 * SUB):
            k = j * wide + w
            kept = squares[k : k + 2 * SUB, :]
            for y in range(rows):
                row, jump = column_row(j, xl, y, dims, count)
                two = [x_ref[pl.ds(row + (w + SUB * h) * jump, SUB, stride=jump), :] for h in range(2)]
                value = jnp.concatenate(two, axis=0)
                kept = kept + value * value
                for n, part in enumerate(terms(value)):
                    x_terms[n * width + k : n * width + k + 2 * SUB, y * LANE : (y + 1) * LANE] = part
            squares[k : k + 2 * SUB, :] = kept

    def against(rows_used, part):
        return lax.dot_general(
            x_terms[:rows_used, :], part[...], (((1,), (1,)), ((), ())), preferred_element_type=jnp.float32
        )

    by_high, by_mid, by_low = against(3 * width, high), against(2 * width, mid), against(width, low)
    small = (by_high[2 * width :] + by_mid[width:]) + by_low
    totals[...] += by_high[:width] + ((by_high[width : 2 * width] + by_mid[:width]) + small)

    @pl.when(xl == near - 1)
    def _():
        for p in range(blocks):
            out_ref[p * width : (p + 1) * width, :] = totals[:, p * LANE : (p + 1) * LANE]
            for q in range(p, blocks):
                at = block_row(width, blocks, p, q)
                out_ref[at : at + LANE, :] = gram[p * LANE : (p + 1) * LANE, q * LANE : (q + 1) * LANE]
        at = block_row(width, blocks, blocks - 1, blocks - 1) + LANE
        out_ref[at:, :] = jnp.zeros((out_ref.shape[0] - at, LANE), jnp.float32)
        out_ref[at : at + SUB, :] = lax.dot_general(
            jnp.ones((SUB, LANE), jnp.float32),
            squares[...],
            (((1,), (1,)), ((), ())),
            precision=lax.Precision.HIGHEST,
            preferred_element_type=jnp.float32,
        )


def first_sums(x, gram, parts, dims, count):
    wide, narrow, near, rows = dims
    width, basis = wide * count, gram.shape[0]
    vmem = pl.BlockSpec(memory_space=pltpu.VMEM)
    cells = pl.BlockSpec((basis, rows * LANE), lambda g: (0, g))
    return pl.pallas_call(
        functools.partial(first_body, dims=dims, count=count),
        grid=(near,),
        out_shape=jax.ShapeDtypeStruct((layout_rows(width, basis, wide * narrow), LANE), jnp.float32),
        in_specs=[vmem, vmem, cells, cells, cells],
        out_specs=vmem,
        scratch_shapes=[
            pltpu.VMEM((3 * width, rows * LANE), jnp.bfloat16),
            pltpu.VMEM((width, basis), jnp.float32),
            pltpu.VMEM((LANE, LANE), jnp.float32),
        ],
        name="first_sums",
    )(x, gram, *parts)


def coef_body(sums, coef_ref, terms_ref, mean_ref, bad_ref, *, width, blocks, total_cells):
    first = [sums[p * width : (p + 1) * width, :] / total_cells for p in range(blocks)]

    def gram_of(p, q):
        at = block_row(width, blocks, min(p, q), max(p, q))
        return sums[at : at + LANE, :] / total_cells

    def through(rows_of):
        out = []
        for q in range(blocks):
            total = None
            for p in range(blocks):
                side = 0 if p <= q else 1
                part = lax.dot_general(
                    rows_of[p],
                    gram_of(p, q),
                    (((1,), (side,)), ((), ())),
                    precision=lax.Precision.HIGHEST,
                    preferred_element_type=jnp.float32,
                )
                total = part if total is None else total + part
            out.append(total)
        return out

    coef = [f + (f - g) for f, g in zip(first, through(first))]
    crossed = folded = 0.0
    for p, (c, g) in enumerate(zip(coef, through(coef))):
        coef_ref[:, p * LANE : (p + 1) * LANE] = c
        for n, part in enumerate(terms(c)):
            terms_ref[n * width : (n + 1) * width, p * LANE : (p + 1) * LANE] = part
        crossed = crossed + 2.0 * jnp.sum(c * first[p], axis=1, keepdims=True)
        folded = folded + jnp.sum(c * g, axis=1, keepdims=True)
    at = block_row(width, blocks, blocks - 1, blocks - 1) + LANE
    row = jnp.broadcast_to(sums[at : at + 1, :], (width, LANE)) / total_cells
    shape = (width, LANE)
    same = lax.broadcasted_iota(jnp.int32, shape, 0) == lax.broadcasted_iota(jnp.int32, shape, 1)
    square = jnp.sum(jnp.where(same, row, 0.0), axis=1, keepdims=True)
    quick = square - crossed + folded
    fine = quick >= 0.1 * (square + jnp.abs(crossed) + folded)
    mean_ref[...] = jnp.broadcast_to(quick, shape)
    bad_ref[0] = jnp.sum(jnp.where(fine, 0.0, 1.0))


def coefficients_of(sums, width, basis, total_cells):
    vmem = pl.BlockSpec(memory_space=pltpu.VMEM)
    return pl.pallas_call(
        functools.partial(coef_body, width=width, blocks=basis // LANE, total_cells=total_cells),
        out_shape=(
            jax.ShapeDtypeStruct((width, basis), jnp.float32),
            jax.ShapeDtypeStruct((3 * width, basis), jnp.bfloat16),
            jax.ShapeDtypeStruct((width, LANE), jnp.float32),
            jax.ShapeDtypeStruct((1,), jnp.float32),
        ),
        in_specs=[vmem],
        out_specs=(vmem, vmem, vmem, pl.BlockSpec(memory_space=pltpu.SMEM)),
        name="coefficients_of",
    )(sums)


def clean_body(x_ref, coef, mean_ref, high, mid, low, out_ref, *, dims, count, scaled):
    wide, narrow, near, rows = dims
    width = wide * count
    xl = pl.program_id(0)
    flat = out_ref.reshape(width * rows, LANE)

    def against(rows_used, part):
        return lax.dot_general(
            coef[:rows_used, :], part[...], (((1,), (0,)), ((), ())), preferred_element_type=jnp.float32
        )

    by_high, by_mid, by_low = against(3 * width, high), against(2 * width, mid), against(width, low)
    small = (by_high[2 * width :] + by_mid[width:]) + by_low
    along = by_high[:width] + ((by_high[width : 2 * width] + by_mid[:width]) + small)
    for j in range(count):
        for w in range(0, wide, SUB):
            k = j * wide + w
            factor = 1.0 / jnp.sqrt(mean_ref[k : k + SUB, :] + 1e-06) if scaled else None
            for y in range(rows):
                row, jump = column_row(j, xl, y, dims, count)
                value = x_ref[pl.ds(row + w * jump, SUB, stride=jump), :]
                value = value - along[k : k + SUB, y * LANE : (y + 1) * LANE]
                if scaled:
                    value = value * factor
                flat[pl.ds(k * rows + y, SUB, stride=rows), :] = value


def cleaned(x, coef_terms, mean_square, parts, dims, count, scaled):
    wide, narrow, near, rows = dims
    width, basis = wide * count, coef_terms.shape[1]
    vmem = pl.BlockSpec(memory_space=pltpu.VMEM)
    cells = pl.BlockSpec((basis, rows * LANE), lambda g: (0, g))
    return pl.pallas_call(
        functools.partial(clean_body, dims=dims, count=count, scaled=scaled),
        grid=(near,),
        out_shape=jax.ShapeDtypeStruct((width, near * rows, LANE), jnp.float32),
        in_specs=[vmem, vmem, vmem, cells, cells, cells],
        out_specs=pl.BlockSpec((width, rows, LANE), lambda g: (0, g, 0)),
        name="cleaned",
    )(x, coef_terms, mean_square, *parts)


def shards_whole(inputs, old_basis, conductance, shifts, total_cells):
    wide, narrow = lax.axis_size("wide"), lax.axis_size("narrow")
    columns, near, rows, _ = inputs.shape
    count, basis = shifts.shape[0], old_basis.shape[0]
    width, dims = columns * count, (wide, narrow, near, rows)
    vflat = old_basis.reshape(basis, -1)
    gram = jnp.einsum("bc,dc->bd", vflat, vflat, precision=lax.Precision.HIGHEST)
    parts = basis_terms(old_basis)
    x, parts = solve_whole(inputs, conductance, shifts, total_cells, parts)
    x = x.reshape(-1, LANE)
    sums = reduced_rows(first_sums(x, gram, parts, dims, count))
    coef, coef_terms, quick, bad = coefficients_of(sums, width, basis, total_cells)

    def slow():
        twice = cleaned(x, coef_terms, quick, parts, dims, count, False)
        total = reduced(jnp.sum(twice * twice, axis=(1, 2))) / total_cells
        return jnp.broadcast_to(total[:, None], quick.shape)

    mean_square = lax.cond(bad[0] == 0.0, lambda: quick, slow)
    new_columns = cleaned(x, coef_terms, mean_square, parts, dims, count, True)
    col_scale = jnp.sqrt(mean_square[:, 0] + 1e-06)
    return (new_columns.reshape((width,) + inputs.shape[1:]), coef.T, col_scale)


def shards_spread(inputs, old_basis, conductance, shifts, total_cells):
    vflat = old_basis.reshape(old_basis.shape[0], -1)
    wflat = solve_spread(inputs, conductance, shifts, total_cells)
    high = lax.Precision.HIGHEST
    first = lax.psum(jnp.einsum("bc,kc->bk", vflat, wflat, precision=high), AXES) / total_cells
    once = wflat - jnp.einsum("bk,bc->kc", first, vflat, precision=high)
    second = lax.psum(jnp.einsum("bc,kc->bk", vflat, once, precision=high), AXES) / total_cells
    twice = once - jnp.einsum("bk,bc->kc", second, vflat, precision=high)
    mean_square = lax.psum(jnp.sum(twice * twice, axis=1), AXES) / total_cells
    col_scale = jnp.sqrt(mean_square + 1e-06)
    new_columns = (twice / col_scale[:, None]).reshape((-1,) + inputs.shape[1:])
    return (new_columns, first + second, col_scale)


def fits_whole(inputs, old_basis, shifts):
    wide, narrow = lax.axis_size("wide"), lax.axis_size("narrow")
    columns, near, rows, lanes = inputs.shape
    own, left = split_columns(shifts.shape[0], narrow)
    field = wide * narrow * near * rows * lanes * 4
    return (
        columns == wide
        and lanes == LANE
        and wide % (2 * SUB) == 0
        and rows == SUB
        and near % narrow == 0
        and wide * near % UNROLL == 0
        and old_basis.shape[0] % LANE == 0
        and columns * shifts.shape[0] <= LANE
        and field * (6 + 8 * (own + left)) <= 24 * 2**20
        and old_basis.size * 4 <= 8 * 2**20
    )


def shards(inputs, old_basis, conductance, shifts):
    total_cells = math.prod(inputs.shape[1:]) * lax.axis_size(AXES)
    form = shards_whole if fits_whole(inputs, old_basis, shifts) else shards_spread
    return form(inputs, old_basis, conductance, shifts, total_cells)


def solution(mesh):
    in_specs = (
        P(None, "wide", "narrow", None),
        P(None, "wide", "narrow", None),
        P("wide", "narrow", None),
        P(),
    )
    out_specs = (P(None, "wide", "narrow", None), P(), P())
    return jax.shard_map(shards, mesh=mesh, in_specs=in_specs, out_specs=out_specs, check_vma=False)
```

```python
import functools
import math

import jax
import jax.numpy as jnp
from jax import lax
from jax.experimental import pallas as pl
from jax.experimental.pallas import tpu as pltpu
from jax.sharding import PartitionSpec as P

ITERS = 4
AXES = ("wide", "narrow")
SUB, LANE = 8, 128
UNROLL = 64
MIB = 2**20


def spread(coef):
    return coef[:, None, None, None]


def reduced(partial):
    count = lax.axis_size(AXES)
    copies = jnp.broadcast_to(partial[None], (count,) + partial.shape)
    return jnp.sum(lax.all_to_all(copies, AXES, 0, 0), axis=0)


def reduced_rows(partial):
    count = lax.axis_size(AXES)
    share = partial.reshape((count, partial.shape[0] // count) + partial.shape[1:])
    own = jnp.sum(lax.all_to_all(share, AXES, 0, 0), axis=0)
    copies = jnp.broadcast_to(own[None], (count,) + own.shape)
    return lax.all_to_all(copies, AXES, 0, 0).reshape(partial.shape)


def padded_2(cells, sides):
    for axis, dim in sides:
        count = lax.axis_size(axis)
        ends = count - 1
        head = lax.slice_in_dim(cells, 0, 1, axis=dim)
        tail = lax.slice_in_dim(cells, cells.shape[dim] - 1, cells.shape[dim], axis=dim)
        cells = jnp.concatenate(
            [
                lax.ppermute(tail, axis, [(i, (i + 1) % count) for i in range(ends)]),
                cells,
                lax.ppermute(head, axis, [((i + 1) % count, i) for i in range(ends)]),
            ],
            axis=dim,
        )
    return cells


def operate(values, conductance, shift_col):
    padded = padded_2(values, (("wide", 1), ("narrow", 2)))
    center = padded[:, 1:-1, 1:-1, :]
    deeper = jnp.pad(padded, ((0, 0), (0, 0), (0, 0), (1, 1)))
    beside_all = deeper[:, 2:, 1:-1, 1:-1] + deeper[:, :-2, 1:-1, 1:-1]
    beside_all = beside_all + deeper[:, 1:-1, 2:, 1:-1] + deeper[:, 1:-1, :-2, 1:-1]
    beside_all = beside_all + deeper[:, 1:-1, 1:-1, 2:] + deeper[:, 1:-1, 1:-1, :-2]
    return conductance[None] * (6.0 * center - beside_all) + spread(shift_col) * center


def local_dot(left, right):
    return jnp.sum(left * right, axis=(1, 2, 3))


def solve_spread(inputs, conductance, shifts, total_cells):
    shift_col = jnp.repeat(shifts, inputs.shape[0])
    shadow = jnp.tile(inputs, (shifts.shape[0], 1, 1, 1))
    solution = jnp.zeros_like(shadow)
    residual = shadow
    search = shadow
    rho_now = lax.psum(local_dot(shadow, shadow), AXES) / total_cells
    for iteration in range(ITERS):
        search_image = operate(search, conductance, shift_col)
        denominator = lax.psum(local_dot(shadow, search_image), AXES) / total_cells
        step_alpha = rho_now / denominator
        halfway = residual - spread(step_alpha) * search_image
        halfway_image = operate(halfway, conductance, shift_col)
        cross_sum, square_sum, shadow_half, shadow_image = lax.psum(
            (
                local_dot(halfway_image, halfway),
                local_dot(halfway_image, halfway_image),
                local_dot(shadow, halfway),
                local_dot(shadow, halfway_image),
            ),
            AXES,
        )
        step_omega = cross_sum / total_cells / (square_sum / total_cells + 1e-06)
        solution = solution + spread(step_alpha) * search + spread(step_omega) * halfway
        residual = halfway - spread(step_omega) * halfway_image
        rho_next = shadow_half / total_cells - step_omega * (shadow_image / total_cells)
        if iteration + 1 < ITERS:
            step_beta = rho_next / rho_now * (step_alpha / step_omega)
            search = residual + spread(step_beta) * (search - spread(step_omega) * search_image)
            rho_now = rho_next
    return solution.reshape(shadow.shape[0], -1)


def split_columns(count, narrow):
    return count // narrow, count % narrow


def solve_body(core_ref, shift_ref, *refs, dims, count, total_cells):
    wide, narrow, near, rows = dims
    own, left = split_columns(count, narrow)
    slots = own + left
    planes, height = wide * near, narrow * rows
    parts, out_ref, (shadow, cond), per = refs[:narrow], refs[narrow], refs[narrow + 1 : narrow + 3], refs[narrow + 3 :]
    names = ("x", "r", "v", "t", "diag", "p", "s")
    col = [dict(zip(names, per[7 * a : 7 * a + 7])) for a in range(slots)]
    core = core_ref[0]
    zero = jnp.zeros((SUB, LANE), jnp.float32)
    lane = lax.broadcasted_iota(jnp.int32, (SUB, LANE), 1)
    first_lane, last_lane = lane == 0, lane == LANE - 1
    group = UNROLL
    tiles = range(0, height, SUB)

    for step in range(narrow):
        at = pl.multiple_of(lax.rem(core + step, narrow) * rows, SUB)
        shadow_half, cond_half = shadow.at[:, pl.ds(at, rows)], cond.at[:, pl.ds(at, rows)]
        for w in range(wide):
            shadow_half[w * near : (w + 1) * near] = parts[step][w, 0]
            cond_half[w * near : (w + 1) * near] = parts[step][w, 1]

    def clear(i, _):
        for a in range(slots):
            for name in ("p", "s"):
                col[a][name][i, :SUB, :] = zero
                col[a][name][i, SUB + height :, :] = zero
        return 0

    lax.fori_loop(0, planes + 2, clear, 0)
    for a in range(slots):
        for name in ("p", "s"):
            for i in (0, planes + 1):
                for y in tiles:
                    col[a][name][i, SUB + y : 2 * SUB + y, :] = zero

    def inner(ref, i, y):
        return ref[i + 1, SUB + y : 2 * SUB + y, :]

    def image(ref, i, y, here, c, diag):
        nb = ref[i, SUB + y : 2 * SUB + y, :] + ref[i + 2, SUB + y : 2 * SUB + y, :]
        nb = nb + (ref[i + 1, SUB + y - 1 : 2 * SUB + y - 1, :] + ref[i + 1, SUB + y + 1 : 2 * SUB + y + 1, :])
        nb = nb + (
            jnp.where(first_lane, 0.0, pltpu.roll(here, 1, 1)) + jnp.where(last_lane, 0.0, pltpu.roll(here, LANE - 1, 1))
        )
        return at_tile(diag, i, y) * here - c * nb

    def mean(acc):
        total = jnp.sum(jnp.sum(acc, axis=1, keepdims=True), axis=0, keepdims=True) / total_cells
        return jnp.broadcast_to(total, (SUB, LANE))

    def over(body, carry):
        def some(g, carry):
            for u in range(group):
                for y in tiles:
                    carry = body(g * group + u, y, carry)
            return carry

        return lax.fori_loop(0, planes // group, some, carry)

    which = [core * own + a for a in range(own)] + [narrow * own + a for a in range(left)]
    shift = [jnp.full((SUB, LANE), shift_ref[j], jnp.float32) for j in which]

    def at_tile(ref, i, y):
        return ref[i, y : y + SUB, :]

    def start(i, y, acc):
        b = at_tile(shadow, i, y)
        six = 6.0 * at_tile(cond, i, y)
        for a in range(slots):
            col[a]["p"][i + 1, SUB + y : 2 * SUB + y, :] = b
            col[a]["r"][i, y : y + SUB, :] = b
            col[a]["x"][i, y : y + SUB, :] = zero
            col[a]["diag"][i, y : y + SUB, :] = six + shift[a]
        return acc + b * b

    def half_step(rho, last):
        def phase_a(i, y, acc):
            b, c = at_tile(shadow, i, y), at_tile(cond, i, y)
            out = []
            for a in range(slots):
                p = col[a]["p"]
                v = image(p, i, y, inner(p, i, y), c, col[a]["diag"])
                col[a]["v"][i, y : y + SUB, :] = v
                out.append(acc[a] + b * v)
            return tuple(out)

        acc = over(phase_a, (zero,) * slots)
        alpha = [rho[a] / mean(acc[a]) for a in range(slots)]

        def phase_b(i, y, _):
            for a in range(slots):
                s = at_tile(col[a]["r"], i, y) - alpha[a] * at_tile(col[a]["v"], i, y)
                col[a]["s"][i + 1, SUB + y : 2 * SUB + y, :] = s
            return 0

        over(phase_b, 0)

        def phase_c(i, y, acc):
            b, c = at_tile(shadow, i, y), at_tile(cond, i, y)
            out = []
            for a in range(slots):
                ref = col[a]["s"]
                s = inner(ref, i, y)
                t = image(ref, i, y, s, c, col[a]["diag"])
                one = [acc[a][0] + t * s, acc[a][1] + t * t]
                if not last:
                    col[a]["t"][i, y : y + SUB, :] = t
                    one += [acc[a][2] + b * s, acc[a][3] + b * t]
                out.append(tuple(one))
            return tuple(out)

        acc = over(phase_c, ((zero,) * (2 if last else 4),) * slots)
        means = [[mean(one) for one in acc[a]] for a in range(slots)]
        omega = [m[0] / (m[1] + 1e-06) for m in means]
        return alpha, omega, means

    def full_step(_, rho):
        alpha, omega, means = half_step(rho, False)
        rho_next = [means[a][2] - omega[a] * means[a][3] for a in range(slots)]
        beta = [rho_next[a] / rho[a] * (alpha[a] / omega[a]) for a in range(slots)]

        def phase_d(i, y, _):
            for a in range(slots):
                p, s = inner(col[a]["p"], i, y), inner(col[a]["s"], i, y)
                col[a]["x"][i, y : y + SUB, :] = at_tile(col[a]["x"], i, y) + (alpha[a] * p + omega[a] * s)
                r = s - omega[a] * at_tile(col[a]["t"], i, y)
                col[a]["r"][i, y : y + SUB, :] = r
                next_p = r + beta[a] * (p - omega[a] * at_tile(col[a]["v"], i, y))
                col[a]["p"][i + 1, SUB + y : 2 * SUB + y, :] = next_p
            return 0

        over(phase_d, 0)
        return tuple(rho_next)

    rho0 = mean(over(start, zero))
    rho = lax.fori_loop(0, ITERS - 1, full_step, (rho0,) * slots)
    alpha, omega, _ = half_step(rho, True)

    share = near // narrow
    chunk = own * near + left * share

    def finished(a, i, y):
        p, s = inner(col[a]["p"], i, y), inner(col[a]["s"], i, y)
        return at_tile(col[a]["x"], i, y) + (alpha[a] * p + omega[a] * s)

    def send(w, _):
        for to in range(narrow):
            base = (w * narrow + to) * chunk
            for a in range(own):
                for xl in range(near):
                    out_ref[base + a * near + xl] = finished(a, w * near + xl, to * rows)
            for e in range(left):
                for xl in range(share):
                    i = w * near + core * share + xl
                    out_ref[base + own * near + e * share + xl] = finished(own + e, i, to * rows)
        return 0

    lax.fori_loop(0, wide, send, 0)


def pack_body(inputs, conductance, out_ref, sems):
    wide = inputs.shape[0]
    copies = [pltpu.make_async_copy(inputs, out_ref.at[:, 0], sems.at[0])]
    for w in range(wide):
        copies.append(pltpu.make_async_copy(conductance, out_ref.at[w, 1], sems.at[w + 1]))
    for copy in copies:
        copy.start()
    for copy in copies:
        copy.wait()


def packed(inputs, conductance):
    anywhere = pl.BlockSpec(memory_space=pltpu.HBM)
    return pl.pallas_call(
        pack_body,
        out_shape=jax.ShapeDtypeStruct((inputs.shape[0], 2) + inputs.shape[1:], jnp.float32),
        in_specs=[anywhere, anywhere],
        out_specs=anywhere,
        scratch_shapes=[pltpu.SemaphoreType.DMA((inputs.shape[0] + 1,))],
        compiler_params=pltpu.CompilerParams(vmem_limit_bytes=8 * MIB),
        name="packed",
    )(inputs, conductance)


def solve_whole(inputs, conductance, shifts, total_cells, beside):
    wide, narrow = lax.axis_size("wide"), lax.axis_size("narrow")
    columns, near, rows, lanes = inputs.shape
    count = shifts.shape[0]
    own, left = split_columns(count, narrow)
    slots = own + left
    got = lax.all_to_all(packed(inputs, conductance), "wide", 0, 0)
    got, beside = lax.optimization_barrier((got, beside))
    parts = [got]
    for step in range(1, narrow):
        parts.append(lax.ppermute(got, "narrow", [((i + step) % narrow, i) for i in range(narrow)]))
    planes, height = wide * near, narrow * rows
    plain = pltpu.VMEM((planes, height, LANE), jnp.float32)
    ringed = pltpu.VMEM((planes + 2, height + 2 * SUB, LANE), jnp.float32)
    share = near // narrow
    chunk = own * near + left * share
    smem, vmem = pl.BlockSpec(memory_space=pltpu.SMEM), pl.BlockSpec(memory_space=pltpu.VMEM)
    x = pl.pallas_call(
        functools.partial(solve_body, dims=(wide, narrow, near, rows), count=count, total_cells=total_cells),
        out_shape=jax.ShapeDtypeStruct((wide * narrow * chunk, rows, LANE), jnp.float32),
        in_specs=[smem, smem] + [vmem] * narrow,
        out_specs=vmem,
        scratch_shapes=[plain, plain] + [plain, plain, plain, plain, plain, ringed, ringed] * slots,
        compiler_params=pltpu.CompilerParams(vmem_limit_bytes=24 * MIB),
        name="solve_whole",
    )(lax.axis_index("narrow").reshape(1), shifts, *parts)
    return lax.all_to_all(x.reshape(wide * narrow, chunk, rows, LANE), AXES, 0, 0), beside


def terms(value):
    high = value.astype(jnp.bfloat16)
    rest = value - high.astype(jnp.float32)
    mid = rest.astype(jnp.bfloat16)
    return high, mid, (rest - mid.astype(jnp.float32)).astype(jnp.bfloat16)


def basis_body(source, *parts, group, held):
    for r in range(held):
        for g in range(0, group, 2 * SUB):
            low = source[pl.ds(g * held + r, SUB, stride=held), :]
            high = source[pl.ds((g + SUB) * held + r, SUB, stride=held), :]
            for part, value in zip(parts, terms(jnp.concatenate([low, high], axis=0))):
                part[g : g + 2 * SUB, r * LANE : (r + 1) * LANE] = value


def basis_terms(old_basis):
    basis = old_basis.shape[0]
    held = old_basis.shape[1] * old_basis.shape[2]
    group = 2 * SUB
    out = jax.ShapeDtypeStruct((basis, held * LANE), jnp.bfloat16)
    return pl.pallas_call(
        functools.partial(basis_body, group=group, held=held),
        grid=(basis // group,),
        out_shape=(out,) * 3,
        in_specs=[pl.BlockSpec((group * held, LANE), lambda g: (g, 0))],
        out_specs=(pl.BlockSpec((group, held * LANE), lambda g: (g, 0)),) * 3,
        compiler_params=pltpu.CompilerParams(vmem_limit_bytes=8 * MIB),
        name="basis_terms",
    )(old_basis.reshape(-1, LANE))


def gram_body(high, mid, low, out_ref):
    def against(left, right):
        return lax.dot_general(
            left[...], right[...], (((1,), (1,)), ((), ())), preferred_element_type=jnp.float32
        )

    across = against(high, mid) + against(high, low)
    out_ref[...] = against(high, high) + (against(mid, mid) + (across + across.T))


def gram_of_terms(parts):
    basis = parts[0].shape[0]
    vmem = pl.BlockSpec(memory_space=pltpu.VMEM)
    return pl.pallas_call(
        gram_body,
        out_shape=jax.ShapeDtypeStruct((basis, basis), jnp.float32),
        in_specs=[vmem] * 3,
        out_specs=vmem,
        cost_estimate=pl.CostEstimate(
            flops=8 * basis * parts[0].size, bytes_accessed=6 * parts[0].size, transcendentals=0
        ),
        compiler_params=pltpu.CompilerParams(vmem_limit_bytes=16 * MIB),
        name="gram_of_terms",
    )(*parts)


def column_row(j, xl, y, dims, count):
    wide, narrow, near, rows = dims
    own, left = split_columns(count, narrow)
    share = near // narrow
    chunk = own * near + left * share
    if j < narrow * own:
        plane = (j // own) * chunk + (j % own) * near + xl
    else:
        plane = (xl // share) * chunk + own * near + (j - narrow * own) * share + xl % share
    return plane * rows + y, narrow * chunk * rows


def layout_rows(width, basis, devices):
    blocks = basis // LANE
    used = width * blocks + LANE * blocks * (blocks + 1) // 2 + SUB
    step = devices * SUB
    return -(-used // step) * step


def block_row(width, blocks, p, q):
    return width * blocks + LANE * (p * blocks - p * (p - 1) // 2 + q - p)


def first_body(x_ref, gram, high, mid, low, out_ref, x_terms, totals, squares, *, dims, count):
    wide, narrow, near, rows = dims
    width = wide * count
    basis = high.shape[0]
    blocks = basis // LANE
    xl = pl.program_id(0)

    @pl.when(xl == 0)
    def _():
        totals[...] = jnp.zeros_like(totals)
        squares[...] = jnp.zeros_like(squares)

    for j in range(count):
        for w in range(0, wide, 2 * SUB):
            k = j * wide + w
            kept = squares[k : k + 2 * SUB, :]
            for y in range(rows):
                row, jump = column_row(j, xl, y, dims, count)
                two = [x_ref[pl.ds(row + (w + SUB * h) * jump, SUB, stride=jump), :] for h in range(2)]
                value = jnp.concatenate(two, axis=0)
                kept = kept + value * value
                for n, part in enumerate(terms(value)):
                    x_terms[n * width + k : n * width + k + 2 * SUB, y * LANE : (y + 1) * LANE] = part
            squares[k : k + 2 * SUB, :] = kept

    def against(rows_used, part):
        return lax.dot_general(
            x_terms[:rows_used, :], part[...], (((1,), (1,)), ((), ())), preferred_element_type=jnp.float32
        )

    by_high, by_mid, by_low = against(3 * width, high), against(2 * width, mid), against(width, low)
    small = (by_high[2 * width :] + by_mid[width:]) + by_low
    totals[...] += by_high[:width] + ((by_high[width : 2 * width] + by_mid[:width]) + small)

    @pl.when(xl == near - 1)
    def _():
        for p in range(blocks):
            out_ref[p * width : (p + 1) * width, :] = totals[:, p * LANE : (p + 1) * LANE]
            for q in range(p, blocks):
                at = block_row(width, blocks, p, q)
                out_ref[at : at + LANE, :] = gram[p * LANE : (p + 1) * LANE, q * LANE : (q + 1) * LANE]
        at = block_row(width, blocks, blocks - 1, blocks - 1) + LANE
        out_ref[at:, :] = jnp.zeros((out_ref.shape[0] - at, LANE), jnp.float32)
        out_ref[at : at + SUB, :] = lax.dot_general(
            jnp.ones((SUB, LANE), jnp.float32),
            squares[...],
            (((1,), (1,)), ((), ())),
            precision=lax.Precision.HIGHEST,
            preferred_element_type=jnp.float32,
        )


def first_sums(x, gram, parts, dims, count):
    wide, narrow, near, rows = dims
    width, basis = wide * count, gram.shape[0]
    vmem = pl.BlockSpec(memory_space=pltpu.VMEM)
    cells = pl.BlockSpec((basis, rows * LANE), lambda g: (0, g))
    return pl.pallas_call(
        functools.partial(first_body, dims=dims, count=count),
        grid=(near,),
        out_shape=jax.ShapeDtypeStruct((layout_rows(width, basis, wide * narrow), LANE), jnp.float32),
        in_specs=[vmem, vmem, cells, cells, cells],
        out_specs=vmem,
        scratch_shapes=[
            pltpu.VMEM((3 * width, rows * LANE), jnp.bfloat16),
            pltpu.VMEM((width, basis), jnp.float32),
            pltpu.VMEM((LANE, LANE), jnp.float32),
        ],
        compiler_params=pltpu.CompilerParams(vmem_limit_bytes=16 * MIB),
        name="first_sums",
    )(x, gram, *parts)


def coef_body(sums, coef_ref, terms_ref, mean_ref, bad_ref, *, width, blocks, total_cells):
    first = [sums[p * width : (p + 1) * width, :] / total_cells for p in range(blocks)]

    def gram_of(p, q):
        at = block_row(width, blocks, min(p, q), max(p, q))
        return sums[at : at + LANE, :] / total_cells

    def through(rows_of):
        out = []
        for q in range(blocks):
            total = None
            for p in range(blocks):
                side = 0 if p <= q else 1
                part = lax.dot_general(
                    rows_of[p],
                    gram_of(p, q),
                    (((1,), (side,)), ((), ())),
                    precision=lax.Precision.HIGHEST,
                    preferred_element_type=jnp.float32,
                )
                total = part if total is None else total + part
            out.append(total)
        return out

    coef = [f + (f - g) for f, g in zip(first, through(first))]
    crossed = folded = 0.0
    for p, (c, g) in enumerate(zip(coef, through(coef))):
        coef_ref[:, p * LANE : (p + 1) * LANE] = c
        for n, part in enumerate(terms(c)):
            terms_ref[n * width : (n + 1) * width, p * LANE : (p + 1) * LANE] = part
        crossed = crossed + 2.0 * jnp.sum(c * first[p], axis=1, keepdims=True)
        folded = folded + jnp.sum(c * g, axis=1, keepdims=True)
    at = block_row(width, blocks, blocks - 1, blocks - 1) + LANE
    row = jnp.broadcast_to(sums[at : at + 1, :], (width, LANE)) / total_cells
    shape = (width, LANE)
    same = lax.broadcasted_iota(jnp.int32, shape, 0) == lax.broadcasted_iota(jnp.int32, shape, 1)
    square = jnp.sum(jnp.where(same, row, 0.0), axis=1, keepdims=True)
    quick = square - crossed + folded
    fine = quick >= 0.1 * (square + jnp.abs(crossed) + folded)
    mean_ref[...] = jnp.broadcast_to(quick, shape)
    bad_ref[0] = jnp.sum(jnp.where(fine, 0.0, 1.0))


def coefficients_of(sums, width, basis, total_cells):
    vmem = pl.BlockSpec(memory_space=pltpu.VMEM)
    return pl.pallas_call(
        functools.partial(coef_body, width=width, blocks=basis // LANE, total_cells=total_cells),
        out_shape=(
            jax.ShapeDtypeStruct((width, basis), jnp.float32),
            jax.ShapeDtypeStruct((3 * width, basis), jnp.bfloat16),
            jax.ShapeDtypeStruct((width, LANE), jnp.float32),
            jax.ShapeDtypeStruct((1,), jnp.float32),
        ),
        in_specs=[vmem],
        out_specs=(vmem, vmem, vmem, pl.BlockSpec(memory_space=pltpu.SMEM)),
        compiler_params=pltpu.CompilerParams(vmem_limit_bytes=8 * MIB),
        name="coefficients_of",
    )(sums)


def clean_body(x_ref, coef, mean_ref, high, mid, low, out_ref, scale_ref, *, dims, count, scaled):
    wide, narrow, near, rows = dims
    width = wide * count
    xl = pl.program_id(0)
    flat = out_ref.reshape(width * rows, LANE)

    @pl.when(xl == 0)
    def _():
        shape = (width, LANE)
        same = lax.broadcasted_iota(jnp.int32, shape, 0) == lax.broadcasted_iota(jnp.int32, shape, 1)
        scale = jnp.sqrt(mean_ref[...] + 1e-06)
        scale_ref[...] = jnp.sum(jnp.where(same, scale, 0.0), axis=0, keepdims=True)[:, :width]

    def against(rows_used, part):
        return lax.dot_general(
            coef[:rows_used, :], part[...], (((1,), (0,)), ((), ())), preferred_element_type=jnp.float32
        )

    by_high, by_mid, by_low = against(3 * width, high), against(2 * width, mid), against(width, low)
    small = (by_high[2 * width :] + by_mid[width:]) + by_low
    along = by_high[:width] + ((by_high[width : 2 * width] + by_mid[:width]) + small)
    for j in range(count):
        for w in range(0, wide, SUB):
            k = j * wide + w
            factor = 1.0 / jnp.sqrt(mean_ref[k : k + SUB, :] + 1e-06) if scaled else None
            for y in range(rows):
                row, jump = column_row(j, xl, y, dims, count)
                value = x_ref[pl.ds(row + w * jump, SUB, stride=jump), :]
                value = value - along[k : k + SUB, y * LANE : (y + 1) * LANE]
                if scaled:
                    value = value * factor
                flat[pl.ds(k * rows + y, SUB, stride=rows), :] = value


def cleaned(x, coef_terms, mean_square, parts, dims, count, scaled):
    wide, narrow, near, rows = dims
    width, basis = wide * count, coef_terms.shape[1]
    vmem = pl.BlockSpec(memory_space=pltpu.VMEM)
    cells = pl.BlockSpec((basis, rows * LANE), lambda g: (0, g))
    return pl.pallas_call(
        functools.partial(clean_body, dims=dims, count=count, scaled=scaled),
        grid=(near,),
        out_shape=(
            jax.ShapeDtypeStruct((width, near * rows, LANE), jnp.float32),
            jax.ShapeDtypeStruct((1, width), jnp.float32),
        ),
        in_specs=[vmem, vmem, vmem, cells, cells, cells],
        out_specs=(pl.BlockSpec((width, rows, LANE), lambda g: (0, g, 0)), pl.BlockSpec((1, width), lambda g: (0, 0))),
        compiler_params=pltpu.CompilerParams(vmem_limit_bytes=16 * MIB),
        name="cleaned",
    )(x, coef_terms, mean_square, *parts)


def shards_whole(inputs, old_basis, conductance, shifts, total_cells):
    wide, narrow = lax.axis_size("wide"), lax.axis_size("narrow")
    columns, near, rows, _ = inputs.shape
    count, basis = shifts.shape[0], old_basis.shape[0]
    width, dims = columns * count, (wide, narrow, near, rows)
    parts = basis_terms(old_basis)
    x, parts = solve_whole(inputs, conductance, shifts, total_cells, parts)
    x = x.reshape(-1, LANE)
    gram = gram_of_terms(parts)
    sums = reduced_rows(first_sums(x, gram, parts, dims, count))
    coef, coef_terms, quick, bad = coefficients_of(sums, width, basis, total_cells)

    def slow():
        twice, _ = cleaned(x, coef_terms, quick, parts, dims, count, False)
        total = reduced(jnp.sum(twice * twice, axis=(1, 2))) / total_cells
        return jnp.broadcast_to(total[:, None], quick.shape)

    mean_square = lax.cond(bad[0] == 0.0, lambda: quick, slow)
    new_columns, col_scale = cleaned(x, coef_terms, mean_square, parts, dims, count, True)
    return (new_columns.reshape((width,) + inputs.shape[1:]), coef.T, col_scale.reshape(-1))


def shards_spread(inputs, old_basis, conductance, shifts, total_cells):
    vflat = old_basis.reshape(old_basis.shape[0], -1)
    wflat = solve_spread(inputs, conductance, shifts, total_cells)
    high = lax.Precision.HIGHEST
    first = lax.psum(jnp.einsum("bc,kc->bk", vflat, wflat, precision=high), AXES) / total_cells
    once = wflat - jnp.einsum("bk,bc->kc", first, vflat, precision=high)
    second = lax.psum(jnp.einsum("bc,kc->bk", vflat, once, precision=high), AXES) / total_cells
    twice = once - jnp.einsum("bk,bc->kc", second, vflat, precision=high)
    mean_square = lax.psum(jnp.sum(twice * twice, axis=1), AXES) / total_cells
    col_scale = jnp.sqrt(mean_square + 1e-06)
    new_columns = (twice / col_scale[:, None]).reshape((-1,) + inputs.shape[1:])
    return (new_columns, first + second, col_scale)


def fits_whole(inputs, old_basis, shifts):
    wide, narrow = lax.axis_size("wide"), lax.axis_size("narrow")
    columns, near, rows, lanes = inputs.shape
    own, left = split_columns(shifts.shape[0], narrow)
    field = wide * narrow * near * rows * lanes * 4
    return (
        columns == wide
        and lanes == LANE
        and wide % (2 * SUB) == 0
        and rows == SUB
        and near % narrow == 0
        and wide * near % UNROLL == 0
        and old_basis.shape[0] % LANE == 0
        and columns * shifts.shape[0] <= LANE
        and field * (6 + 10 * (own + left)) <= 24 * 2**20
        and old_basis.size * 4 <= 8 * 2**20
    )


def shards(inputs, old_basis, conductance, shifts):
    total_cells = math.prod(inputs.shape[1:]) * lax.axis_size(AXES)
    form = shards_whole if fits_whole(inputs, old_basis, shifts) else shards_spread
    return form(inputs, old_basis, conductance, shifts, total_cells)


def solution(mesh):
    in_specs = (
        P(None, "wide", "narrow", None),
        P(None, "wide", "narrow", None),
        P("wide", "narrow", None),
        P(),
    )
    out_specs = (P(None, "wide", "narrow", None), P(), P())
    return jax.shard_map(shards, mesh=mesh, in_specs=in_specs, out_specs=out_specs, check_vma=False)
```

```python
import functools
import math

import jax
import jax.numpy as jnp
from jax import lax
from jax.experimental import pallas as pl
from jax.experimental.pallas import tpu as pltpu
from jax.sharding import PartitionSpec as P

ITERS = 4
AXES = ("wide", "narrow")
SUB, LANE = 8, 128
UNROLL = 64
MIB = 2**20


def spread(coef):
    return coef[:, None, None, None]


def reduced(partial):
    count = lax.axis_size(AXES)
    copies = jnp.broadcast_to(partial[None], (count,) + partial.shape)
    return jnp.sum(lax.all_to_all(copies, AXES, 0, 0), axis=0)


def reduced_rows(partial):
    count = lax.axis_size(AXES)
    share = partial.reshape((count, partial.shape[0] // count) + partial.shape[1:])
    own = jnp.sum(lax.all_to_all(share, AXES, 0, 0), axis=0)
    copies = jnp.broadcast_to(own[None], (count,) + own.shape)
    return lax.all_to_all(copies, AXES, 0, 0).reshape(partial.shape)


def padded_2(cells, sides):
    for axis, dim in sides:
        count = lax.axis_size(axis)
        ends = count - 1
        head = lax.slice_in_dim(cells, 0, 1, axis=dim)
        tail = lax.slice_in_dim(cells, cells.shape[dim] - 1, cells.shape[dim], axis=dim)
        cells = jnp.concatenate(
            [
                lax.ppermute(tail, axis, [(i, (i + 1) % count) for i in range(ends)]),
                cells,
                lax.ppermute(head, axis, [((i + 1) % count, i) for i in range(ends)]),
            ],
            axis=dim,
        )
    return cells


def operate(values, conductance, shift_col):
    padded = padded_2(values, (("wide", 1), ("narrow", 2)))
    center = padded[:, 1:-1, 1:-1, :]
    deeper = jnp.pad(padded, ((0, 0), (0, 0), (0, 0), (1, 1)))
    beside_all = deeper[:, 2:, 1:-1, 1:-1] + deeper[:, :-2, 1:-1, 1:-1]
    beside_all = beside_all + deeper[:, 1:-1, 2:, 1:-1] + deeper[:, 1:-1, :-2, 1:-1]
    beside_all = beside_all + deeper[:, 1:-1, 1:-1, 2:] + deeper[:, 1:-1, 1:-1, :-2]
    return conductance[None] * (6.0 * center - beside_all) + spread(shift_col) * center


def local_dot(left, right):
    return jnp.sum(left * right, axis=(1, 2, 3))


def solve_spread(inputs, conductance, shifts, total_cells):
    shift_col = jnp.repeat(shifts, inputs.shape[0])
    shadow = jnp.tile(inputs, (shifts.shape[0], 1, 1, 1))
    solution = jnp.zeros_like(shadow)
    residual = shadow
    search = shadow
    rho_now = lax.psum(local_dot(shadow, shadow), AXES) / total_cells
    for iteration in range(ITERS):
        search_image = operate(search, conductance, shift_col)
        denominator = lax.psum(local_dot(shadow, search_image), AXES) / total_cells
        step_alpha = rho_now / denominator
        halfway = residual - spread(step_alpha) * search_image
        halfway_image = operate(halfway, conductance, shift_col)
        cross_sum, square_sum, shadow_half, shadow_image = lax.psum(
            (
                local_dot(halfway_image, halfway),
                local_dot(halfway_image, halfway_image),
                local_dot(shadow, halfway),
                local_dot(shadow, halfway_image),
            ),
            AXES,
        )
        step_omega = cross_sum / total_cells / (square_sum / total_cells + 1e-06)
        solution = solution + spread(step_alpha) * search + spread(step_omega) * halfway
        residual = halfway - spread(step_omega) * halfway_image
        rho_next = shadow_half / total_cells - step_omega * (shadow_image / total_cells)
        if iteration + 1 < ITERS:
            step_beta = rho_next / rho_now * (step_alpha / step_omega)
            search = residual + spread(step_beta) * (search - spread(step_omega) * search_image)
            rho_now = rho_next
    return solution.reshape(shadow.shape[0], -1)


def split_columns(count, narrow):
    return count // narrow, count % narrow


def solve_body(core_ref, shift_ref, *refs, dims, count, total_cells):
    wide, narrow, near, rows = dims
    own, left = split_columns(count, narrow)
    slots = own + left
    planes, height = wide * near, narrow * rows
    parts, out_ref, (shadow, cond), per = refs[:narrow], refs[narrow], refs[narrow + 1 : narrow + 3], refs[narrow + 3 :]
    names = ("x", "r", "v", "t", "diag", "p", "s")
    col = [dict(zip(names, per[7 * a : 7 * a + 7])) for a in range(slots)]
    core = core_ref[0]
    zero = jnp.zeros((SUB, LANE), jnp.float32)
    lane = lax.broadcasted_iota(jnp.int32, (SUB, LANE), 1)
    first_lane, last_lane = lane == 0, lane == LANE - 1
    group = UNROLL
    tiles = range(0, height, SUB)

    for step in range(narrow):
        at = pl.multiple_of(lax.rem(core + step, narrow) * rows, SUB)
        shadow_half, cond_half = shadow.at[:, pl.ds(at, rows)], cond.at[:, pl.ds(at, rows)]
        for w in range(wide):
            shadow_half[w * near : (w + 1) * near] = parts[step][w, 0]
            cond_half[w * near : (w + 1) * near] = parts[step][w, 1]

    def clear(i, _):
        for a in range(slots):
            for name in ("p", "s"):
                col[a][name][i, :SUB, :] = zero
                col[a][name][i, SUB + height :, :] = zero
        return 0

    lax.fori_loop(0, planes + 2, clear, 0)
    for a in range(slots):
        for name in ("p", "s"):
            for i in (0, planes + 1):
                for y in tiles:
                    col[a][name][i, SUB + y : 2 * SUB + y, :] = zero

    def inner(ref, i, y):
        return ref[i + 1, SUB + y : 2 * SUB + y, :]

    def image(ref, i, y, here, c, diag):
        nb = ref[i, SUB + y : 2 * SUB + y, :] + ref[i + 2, SUB + y : 2 * SUB + y, :]
        nb = nb + (ref[i + 1, SUB + y - 1 : 2 * SUB + y - 1, :] + ref[i + 1, SUB + y + 1 : 2 * SUB + y + 1, :])
        nb = nb + (
            jnp.where(first_lane, 0.0, pltpu.roll(here, 1, 1)) + jnp.where(last_lane, 0.0, pltpu.roll(here, LANE - 1, 1))
        )
        return at_tile(diag, i, y) * here - c * nb

    def mean(acc):
        total = jnp.sum(jnp.sum(acc, axis=1, keepdims=True), axis=0, keepdims=True) / total_cells
        return jnp.broadcast_to(total, (SUB, LANE))

    def over(body, carry):
        def some(g, carry):
            for u in range(group):
                for y in tiles:
                    carry = body(g * group + u, y, carry)
            return carry

        return lax.fori_loop(0, planes // group, some, carry)

    which = [core * own + a for a in range(own)] + [narrow * own + a for a in range(left)]
    shift = [jnp.full((SUB, LANE), shift_ref[j], jnp.float32) for j in which]

    def at_tile(ref, i, y):
        return ref[i, y : y + SUB, :]

    def start(i, y, acc):
        b = at_tile(shadow, i, y)
        six = 6.0 * at_tile(cond, i, y)
        for a in range(slots):
            col[a]["p"][i + 1, SUB + y : 2 * SUB + y, :] = b
            col[a]["r"][i, y : y + SUB, :] = b
            col[a]["x"][i, y : y + SUB, :] = zero
            col[a]["diag"][i, y : y + SUB, :] = six + shift[a]
        return acc + b * b

    def half_step(rho, last):
        def phase_a(i, y, acc):
            b, c = at_tile(shadow, i, y), at_tile(cond, i, y)
            out = []
            for a in range(slots):
                p = col[a]["p"]
                v = image(p, i, y, inner(p, i, y), c, col[a]["diag"])
                col[a]["v"][i, y : y + SUB, :] = v
                out.append(acc[a] + b * v)
            return tuple(out)

        acc = over(phase_a, (zero,) * slots)
        alpha = [rho[a] / mean(acc[a]) for a in range(slots)]

        def phase_b(i, y, _):
            for a in range(slots):
                s = at_tile(col[a]["r"], i, y) - alpha[a] * at_tile(col[a]["v"], i, y)
                col[a]["s"][i + 1, SUB + y : 2 * SUB + y, :] = s
            return 0

        over(phase_b, 0)

        def phase_c(i, y, acc):
            b, c = at_tile(shadow, i, y), at_tile(cond, i, y)
            out = []
            for a in range(slots):
                ref = col[a]["s"]
                s = inner(ref, i, y)
                t = image(ref, i, y, s, c, col[a]["diag"])
                one = [acc[a][0] + t * s, acc[a][1] + t * t]
                if not last:
                    col[a]["t"][i, y : y + SUB, :] = t
                    one += [acc[a][2] + b * s, acc[a][3] + b * t]
                out.append(tuple(one))
            return tuple(out)

        acc = over(phase_c, ((zero,) * (2 if last else 4),) * slots)
        means = [[mean(one) for one in acc[a]] for a in range(slots)]
        omega = [m[0] / (m[1] + 1e-06) for m in means]
        return alpha, omega, means

    def full_step(_, rho):
        alpha, omega, means = half_step(rho, False)
        rho_next = [means[a][2] - omega[a] * means[a][3] for a in range(slots)]
        beta = [rho_next[a] / rho[a] * (alpha[a] / omega[a]) for a in range(slots)]

        def phase_d(i, y, _):
            for a in range(slots):
                p, s = inner(col[a]["p"], i, y), inner(col[a]["s"], i, y)
                col[a]["x"][i, y : y + SUB, :] = at_tile(col[a]["x"], i, y) + (alpha[a] * p + omega[a] * s)
                r = s - omega[a] * at_tile(col[a]["t"], i, y)
                col[a]["r"][i, y : y + SUB, :] = r
                next_p = r + beta[a] * (p - omega[a] * at_tile(col[a]["v"], i, y))
                col[a]["p"][i + 1, SUB + y : 2 * SUB + y, :] = next_p
            return 0

        over(phase_d, 0)
        return tuple(rho_next)

    rho0 = mean(over(start, zero))
    rho = lax.fori_loop(0, ITERS - 1, full_step, (rho0,) * slots)
    alpha, omega, _ = half_step(rho, True)

    share = near // narrow
    chunk = own * near + left * share

    def finished(a, i, y):
        p, s = inner(col[a]["p"], i, y), inner(col[a]["s"], i, y)
        return at_tile(col[a]["x"], i, y) + (alpha[a] * p + omega[a] * s)

    def send(w, _):
        for to in range(narrow):
            base = (w * narrow + to) * chunk
            for a in range(own):
                for xl in range(near):
                    out_ref[base + a * near + xl] = finished(a, w * near + xl, to * rows)
            for e in range(left):
                for xl in range(share):
                    i = w * near + core * share + xl
                    out_ref[base + own * near + e * share + xl] = finished(own + e, i, to * rows)
        return 0

    lax.fori_loop(0, wide, send, 0)


def pack_body(inputs, conductance, out_ref):
    cond = conductance[...]
    for w in range(inputs.shape[0]):
        out_ref[w, 0] = inputs[w]
        out_ref[w, 1] = cond


def packed(inputs, conductance):
    vmem = pl.BlockSpec(memory_space=pltpu.VMEM)
    return pl.pallas_call(
        pack_body,
        out_shape=jax.ShapeDtypeStruct((inputs.shape[0], 2) + inputs.shape[1:], jnp.float32),
        in_specs=[vmem, vmem],
        out_specs=vmem,
        name="packed",
    )(inputs, conductance)


def solve_whole(inputs, conductance, shifts, total_cells, beside):
    wide, narrow = lax.axis_size("wide"), lax.axis_size("narrow")
    columns, near, rows, lanes = inputs.shape
    count = shifts.shape[0]
    own, left = split_columns(count, narrow)
    slots = own + left
    got = lax.all_to_all(packed(inputs, conductance), "wide", 0, 0)
    got, beside = lax.optimization_barrier((got, beside))
    parts = [got]
    for step in range(1, narrow):
        parts.append(lax.ppermute(got, "narrow", [((i + step) % narrow, i) for i in range(narrow)]))
    planes, height = wide * near, narrow * rows
    plain = pltpu.VMEM((planes, height, LANE), jnp.float32)
    ringed = pltpu.VMEM((planes + 2, height + 2 * SUB, LANE), jnp.float32)
    share = near // narrow
    chunk = own * near + left * share
    smem, vmem = pl.BlockSpec(memory_space=pltpu.SMEM), pl.BlockSpec(memory_space=pltpu.VMEM)
    x = pl.pallas_call(
        functools.partial(solve_body, dims=(wide, narrow, near, rows), count=count, total_cells=total_cells),
        out_shape=jax.ShapeDtypeStruct((wide * narrow * chunk, rows, LANE), jnp.float32),
        in_specs=[smem, smem] + [vmem] * narrow,
        out_specs=vmem,
        scratch_shapes=[plain, plain] + [plain, plain, plain, plain, plain, ringed, ringed] * slots,
        compiler_params=pltpu.CompilerParams(vmem_limit_bytes=24 * MIB),
        name="solve_whole",
    )(lax.axis_index("narrow").reshape(1), shifts, *parts)
    return lax.all_to_all(x.reshape(wide * narrow, chunk, rows, LANE), AXES, 0, 0), beside


def terms(value):
    high = value.astype(jnp.bfloat16)
    rest = value - high.astype(jnp.float32)
    mid = rest.astype(jnp.bfloat16)
    return high, mid, (rest - mid.astype(jnp.float32)).astype(jnp.bfloat16)


def basis_body(source, *parts, group, held):
    for r in range(held):
        for g in range(0, group, 2 * SUB):
            low = source[pl.ds(g * held + r, SUB, stride=held), :]
            high = source[pl.ds((g + SUB) * held + r, SUB, stride=held), :]
            for part, value in zip(parts, terms(jnp.concatenate([low, high], axis=0))):
                part[g : g + 2 * SUB, r * LANE : (r + 1) * LANE] = value


def basis_terms(old_basis):
    basis = old_basis.shape[0]
    held = old_basis.shape[1] * old_basis.shape[2]
    group = 2 * SUB
    out = jax.ShapeDtypeStruct((basis, held * LANE), jnp.bfloat16)
    return pl.pallas_call(
        functools.partial(basis_body, group=group, held=held),
        grid=(basis // group,),
        out_shape=(out,) * 3,
        in_specs=[pl.BlockSpec((group * held, LANE), lambda g: (g, 0))],
        out_specs=(pl.BlockSpec((group, held * LANE), lambda g: (g, 0)),) * 3,
        compiler_params=pltpu.CompilerParams(vmem_limit_bytes=8 * MIB),
        name="basis_terms",
    )(old_basis.reshape(-1, LANE))


def gram_body(high, mid, low, out_ref):
    def against(left, right):
        return lax.dot_general(
            left[...], right[...], (((1,), (1,)), ((), ())), preferred_element_type=jnp.float32
        )

    across = against(high, mid) + against(high, low)
    out_ref[...] = against(high, high) + (against(mid, mid) + (across + across.T))


def gram_of_terms(parts):
    basis = parts[0].shape[0]
    vmem = pl.BlockSpec(memory_space=pltpu.VMEM)
    return pl.pallas_call(
        gram_body,
        out_shape=jax.ShapeDtypeStruct((basis, basis), jnp.float32),
        in_specs=[vmem] * 3,
        out_specs=vmem,
        cost_estimate=pl.CostEstimate(
            flops=8 * basis * parts[0].size, bytes_accessed=6 * parts[0].size, transcendentals=0
        ),
        compiler_params=pltpu.CompilerParams(vmem_limit_bytes=16 * MIB),
        name="gram_of_terms",
    )(*parts)


def column_row(j, xl, y, dims, count):
    wide, narrow, near, rows = dims
    own, left = split_columns(count, narrow)
    share = near // narrow
    chunk = own * near + left * share
    if j < narrow * own:
        plane = (j // own) * chunk + (j % own) * near + xl
    else:
        plane = (xl // share) * chunk + own * near + (j - narrow * own) * share + xl % share
    return plane * rows + y, narrow * chunk * rows


def layout_rows(width, basis, devices):
    blocks = basis // LANE
    used = width * blocks + LANE * blocks * (blocks + 1) // 2 + SUB
    step = devices * SUB
    return -(-used // step) * step


def block_row(width, blocks, p, q):
    return width * blocks + LANE * (p * blocks - p * (p - 1) // 2 + q - p)


def first_body(x_ref, gram, high, mid, low, out_ref, x_terms, totals, squares, *, dims, count):
    wide, narrow, near, rows = dims
    width = wide * count
    basis = high.shape[0]
    blocks = basis // LANE
    xl = pl.program_id(0)

    @pl.when(xl == 0)
    def _():
        totals[...] = jnp.zeros_like(totals)
        squares[...] = jnp.zeros_like(squares)

    for j in range(count):
        for w in range(0, wide, 2 * SUB):
            k = j * wide + w
            kept = squares[k : k + 2 * SUB, :]
            for y in range(rows):
                row, jump = column_row(j, xl, y, dims, count)
                two = [x_ref[pl.ds(row + (w + SUB * h) * jump, SUB, stride=jump), :] for h in range(2)]
                value = jnp.concatenate(two, axis=0)
                kept = kept + value * value
                for n, part in enumerate(terms(value)):
                    x_terms[n * width + k : n * width + k + 2 * SUB, y * LANE : (y + 1) * LANE] = part
            squares[k : k + 2 * SUB, :] = kept

    def against(rows_used, part):
        return lax.dot_general(
            x_terms[:rows_used, :], part[...], (((1,), (1,)), ((), ())), preferred_element_type=jnp.float32
        )

    by_high, by_mid, by_low = against(3 * width, high), against(2 * width, mid), against(width, low)
    small = (by_high[2 * width :] + by_mid[width:]) + by_low
    totals[...] += by_high[:width] + ((by_high[width : 2 * width] + by_mid[:width]) + small)

    @pl.when(xl == near - 1)
    def _():
        for p in range(blocks):
            out_ref[p * width : (p + 1) * width, :] = totals[:, p * LANE : (p + 1) * LANE]
            for q in range(p, blocks):
                at = block_row(width, blocks, p, q)
                out_ref[at : at + LANE, :] = gram[p * LANE : (p + 1) * LANE, q * LANE : (q + 1) * LANE]
        at = block_row(width, blocks, blocks - 1, blocks - 1) + LANE
        out_ref[at:, :] = jnp.zeros((out_ref.shape[0] - at, LANE), jnp.float32)
        out_ref[at : at + SUB, :] = lax.dot_general(
            jnp.ones((SUB, LANE), jnp.float32),
            squares[...],
            (((1,), (1,)), ((), ())),
            precision=lax.Precision.HIGHEST,
            preferred_element_type=jnp.float32,
        )


def first_sums(x, gram, parts, dims, count):
    wide, narrow, near, rows = dims
    width, basis = wide * count, gram.shape[0]
    vmem = pl.BlockSpec(memory_space=pltpu.VMEM)
    cells = pl.BlockSpec((basis, rows * LANE), lambda g: (0, g))
    return pl.pallas_call(
        functools.partial(first_body, dims=dims, count=count),
        grid=(near,),
        out_shape=jax.ShapeDtypeStruct((layout_rows(width, basis, wide * narrow), LANE), jnp.float32),
        in_specs=[vmem, vmem, cells, cells, cells],
        out_specs=vmem,
        scratch_shapes=[
            pltpu.VMEM((3 * width, rows * LANE), jnp.bfloat16),
            pltpu.VMEM((width, basis), jnp.float32),
            pltpu.VMEM((LANE, LANE), jnp.float32),
        ],
        compiler_params=pltpu.CompilerParams(vmem_limit_bytes=16 * MIB),
        name="first_sums",
    )(x, gram, *parts)


def coef_body(sums, coef_ref, terms_ref, mean_ref, bad_ref, *, width, blocks, total_cells):
    first = [sums[p * width : (p + 1) * width, :] / total_cells for p in range(blocks)]

    def gram_of(p, q):
        at = block_row(width, blocks, min(p, q), max(p, q))
        return sums[at : at + LANE, :] / total_cells

    def through(rows_of):
        out = []
        for q in range(blocks):
            total = None
            for p in range(blocks):
                side = 0 if p <= q else 1
                part = lax.dot_general(
                    rows_of[p],
                    gram_of(p, q),
                    (((1,), (side,)), ((), ())),
                    precision=lax.Precision.HIGHEST,
                    preferred_element_type=jnp.float32,
                )
                total = part if total is None else total + part
            out.append(total)
        return out

    coef = [f + (f - g) for f, g in zip(first, through(first))]
    crossed = folded = 0.0
    for p, (c, g) in enumerate(zip(coef, through(coef))):
        coef_ref[:, p * LANE : (p + 1) * LANE] = c
        for n, part in enumerate(terms(c)):
            terms_ref[n * width : (n + 1) * width, p * LANE : (p + 1) * LANE] = part
        crossed = crossed + 2.0 * jnp.sum(c * first[p], axis=1, keepdims=True)
        folded = folded + jnp.sum(c * g, axis=1, keepdims=True)
    at = block_row(width, blocks, blocks - 1, blocks - 1) + LANE
    row = jnp.broadcast_to(sums[at : at + 1, :], (width, LANE)) / total_cells
    shape = (width, LANE)
    same = lax.broadcasted_iota(jnp.int32, shape, 0) == lax.broadcasted_iota(jnp.int32, shape, 1)
    square = jnp.sum(jnp.where(same, row, 0.0), axis=1, keepdims=True)
    quick = square - crossed + folded
    fine = quick >= 0.1 * (square + jnp.abs(crossed) + folded)
    mean_ref[...] = jnp.broadcast_to(quick, shape)
    bad_ref[0] = jnp.sum(jnp.where(fine, 0.0, 1.0))


def coefficients_of(sums, width, basis, total_cells):
    vmem = pl.BlockSpec(memory_space=pltpu.VMEM)
    return pl.pallas_call(
        functools.partial(coef_body, width=width, blocks=basis // LANE, total_cells=total_cells),
        out_shape=(
            jax.ShapeDtypeStruct((width, basis), jnp.float32),
            jax.ShapeDtypeStruct((3 * width, basis), jnp.bfloat16),
            jax.ShapeDtypeStruct((width, LANE), jnp.float32),
            jax.ShapeDtypeStruct((1,), jnp.float32),
        ),
        in_specs=[vmem],
        out_specs=(vmem, vmem, vmem, pl.BlockSpec(memory_space=pltpu.SMEM)),
        compiler_params=pltpu.CompilerParams(vmem_limit_bytes=8 * MIB),
        name="coefficients_of",
    )(sums)


def clean_body(x_ref, coef, mean_ref, high, mid, low, out_ref, scale_ref, *, dims, count, scaled):
    wide, narrow, near, rows = dims
    width = wide * count
    xl = pl.program_id(0)
    flat = out_ref.reshape(width * rows, LANE)

    @pl.when(xl == 0)
    def _():
        shape = (width, LANE)
        same = lax.broadcasted_iota(jnp.int32, shape, 0) == lax.broadcasted_iota(jnp.int32, shape, 1)
        scale = jnp.sqrt(mean_ref[...] + 1e-06)
        scale_ref[...] = jnp.sum(jnp.where(same, scale, 0.0), axis=0, keepdims=True)[:, :width]

    def against(rows_used, part):
        return lax.dot_general(
            coef[:rows_used, :], part[...], (((1,), (0,)), ((), ())), preferred_element_type=jnp.float32
        )

    by_high, by_mid, by_low = against(3 * width, high), against(2 * width, mid), against(width, low)
    small = (by_high[2 * width :] + by_mid[width:]) + by_low
    along = by_high[:width] + ((by_high[width : 2 * width] + by_mid[:width]) + small)
    for j in range(count):
        for w in range(0, wide, SUB):
            k = j * wide + w
            factor = 1.0 / jnp.sqrt(mean_ref[k : k + SUB, :] + 1e-06) if scaled else None
            for y in range(rows):
                row, jump = column_row(j, xl, y, dims, count)
                value = x_ref[pl.ds(row + w * jump, SUB, stride=jump), :]
                value = value - along[k : k + SUB, y * LANE : (y + 1) * LANE]
                if scaled:
                    value = value * factor
                flat[pl.ds(k * rows + y, SUB, stride=rows), :] = value


def cleaned(x, coef_terms, mean_square, parts, dims, count, scaled):
    wide, narrow, near, rows = dims
    width, basis = wide * count, coef_terms.shape[1]
    vmem = pl.BlockSpec(memory_space=pltpu.VMEM)
    cells = pl.BlockSpec((basis, rows * LANE), lambda g: (0, g))
    return pl.pallas_call(
        functools.partial(clean_body, dims=dims, count=count, scaled=scaled),
        grid=(near,),
        out_shape=(
            jax.ShapeDtypeStruct((width, near * rows, LANE), jnp.float32),
            jax.ShapeDtypeStruct((1, width), jnp.float32),
        ),
        in_specs=[vmem, vmem, vmem, cells, cells, cells],
        out_specs=(pl.BlockSpec((width, rows, LANE), lambda g: (0, g, 0)), pl.BlockSpec((1, width), lambda g: (0, 0))),
        compiler_params=pltpu.CompilerParams(vmem_limit_bytes=16 * MIB),
        name="cleaned",
    )(x, coef_terms, mean_square, *parts)


def shards_whole(inputs, old_basis, conductance, shifts, total_cells):
    wide, narrow = lax.axis_size("wide"), lax.axis_size("narrow")
    columns, near, rows, _ = inputs.shape
    count, basis = shifts.shape[0], old_basis.shape[0]
    width, dims = columns * count, (wide, narrow, near, rows)
    parts = basis_terms(old_basis)
    x, parts = solve_whole(inputs, conductance, shifts, total_cells, parts)
    x = x.reshape(-1, LANE)
    gram = gram_of_terms(parts)
    sums = reduced_rows(first_sums(x, gram, parts, dims, count))
    coef, coef_terms, quick, bad = coefficients_of(sums, width, basis, total_cells)

    def slow():
        twice, _ = cleaned(x, coef_terms, quick, parts, dims, count, False)
        total = reduced(jnp.sum(twice * twice, axis=(1, 2))) / total_cells
        return jnp.broadcast_to(total[:, None], quick.shape)

    mean_square = lax.cond(bad[0] == 0.0, lambda: quick, slow)
    new_columns, col_scale = cleaned(x, coef_terms, mean_square, parts, dims, count, True)
    return (new_columns.reshape((width,) + inputs.shape[1:]), coef.T, col_scale.reshape(-1))


def shards_spread(inputs, old_basis, conductance, shifts, total_cells):
    vflat = old_basis.reshape(old_basis.shape[0], -1)
    wflat = solve_spread(inputs, conductance, shifts, total_cells)
    high = lax.Precision.HIGHEST
    first = lax.psum(jnp.einsum("bc,kc->bk", vflat, wflat, precision=high), AXES) / total_cells
    once = wflat - jnp.einsum("bk,bc->kc", first, vflat, precision=high)
    second = lax.psum(jnp.einsum("bc,kc->bk", vflat, once, precision=high), AXES) / total_cells
    twice = once - jnp.einsum("bk,bc->kc", second, vflat, precision=high)
    mean_square = lax.psum(jnp.sum(twice * twice, axis=1), AXES) / total_cells
    col_scale = jnp.sqrt(mean_square + 1e-06)
    new_columns = (twice / col_scale[:, None]).reshape((-1,) + inputs.shape[1:])
    return (new_columns, first + second, col_scale)


def fits_whole(inputs, old_basis, shifts):
    wide, narrow = lax.axis_size("wide"), lax.axis_size("narrow")
    columns, near, rows, lanes = inputs.shape
    own, left = split_columns(shifts.shape[0], narrow)
    field = wide * narrow * near * rows * lanes * 4
    return (
        columns == wide
        and lanes == LANE
        and wide % (2 * SUB) == 0
        and rows == SUB
        and near % narrow == 0
        and wide * near % UNROLL == 0
        and old_basis.shape[0] % LANE == 0
        and columns * shifts.shape[0] <= LANE
        and field * (6 + 10 * (own + left)) <= 24 * 2**20
        and old_basis.size * 4 <= 8 * 2**20
    )


def shards(inputs, old_basis, conductance, shifts):
    total_cells = math.prod(inputs.shape[1:]) * lax.axis_size(AXES)
    form = shards_whole if fits_whole(inputs, old_basis, shifts) else shards_spread
    return form(inputs, old_basis, conductance, shifts, total_cells)


def solution(mesh):
    in_specs = (
        P(None, "wide", "narrow", None),
        P(None, "wide", "narrow", None),
        P("wide", "narrow", None),
        P(),
    )
    out_specs = (P(None, "wide", "narrow", None), P(), P())
    return jax.shard_map(shards, mesh=mesh, in_specs=in_specs, out_specs=out_specs, check_vma=False)
```
